256 devices in a mesh: row: 16 (over x, z_lo, core), col: 16 (over z_hi, y).
Axes of the slice: x: 4, y: 4, z: 8 (z_hi: 4, z_lo: 2; z = z_hi * 2 + z_lo), core: 2. Of those that a mesh axis runs over, the one named last changes fastest.
Arguments:
- tokens: bfloat16 [2048, 4096], P('col', 'row'), may hold values from -12 to 12
- target: bfloat16 [2048, 4096], P('col', 'row'), may hold values from -6 to 6
- gate_weight: bfloat16 [4096, 5504], P('row', 'col'), may hold values from -0.09375 to 0.09375
- up_weight: bfloat16 [4096, 5504], P('row', 'col'), may hold values from -0.09375 to 0.09375
- down_weight: bfloat16 [5504, 4096], P('col', 'row'), may hold values from -0.078125 to 0.078125
- probe_gate: int32 [4096, 5504], P('row', 'col'), may hold values from 0 to 1
- probe_up: int32 [4096, 5504], P('row', 'col'), may hold values from 0 to 1
- probe_down: int32 [5504, 4096], P('col', 'row'), may hold values from 0 to 1
- first_gate: float32 [4096, 5504], P('row', 'col'), may hold values from -1.8 to 1.8
- first_up: float32 [4096, 5504], P('row', 'col'), may hold values from -1.8 to 1.8
- first_down: float32 [5504, 4096], P('col', 'row'), may hold values from -1.8 to 1.8
- second_gate: float32 [4096, 5504], P('row', 'col'), may hold values from 0.01 to 0.2
- second_up: float32 [4096, 5504], P('row', 'col'), may hold values from 0.01 to 0.2
- second_down: float32 [5504, 4096], P('col', 'row'), may hold values from 0.01 to 0.2
Outputs:
- new_first_gate: float32 [4096, 5504], P('row', 'col')
- new_first_up: float32 [4096, 5504], P('row', 'col')
- new_first_down: float32 [5504, 4096], P('col', 'row')
- new_second_gate: float32 [4096, 5504], P('row', 'col')
- new_second_up: float32 [4096, 5504], P('row', 'col')
- new_second_down: float32 [5504, 4096], P('col', 'row')
- update_gate: float32 [4096, 5504], P('row', 'col')
- update_up: float32 [4096, 5504], P('row', 'col')
- update_down: float32 [5504, 4096], P('col', 'row')
The draws below stay inside these ranges and needn't reach their ends.
Inputs may be any that keep to these rules, and one draw needn't show every extreme that they name: `probe_gate`: probe bits; the probe is 2 p - 1. `probe_up`: probe bits; the probe is 2 p - 1. `probe_down`: probe bits; the probe is 2 p - 1.
All inputs are finite; a program needn't handle non-finite values.
Results may differ from the reference program's by a relative error of at most 0.038.
Values may be sent and summed in bfloat16 or wider, within the bound.
A program may use at most 128 MiB of HBM per device.

```python
import math
import jax
import jax.numpy as jnp
from jax import lax

D = 4096
FF = 5504
STEP = 10
TOKENS = 2048
N_ROW = 16
N_COL = 16


def draw_tokens(key, part):
    first_key, second_key = jax.random.split(jax.random.fold_in(key, 17), 2)
    position = jnp.arange(D, dtype=jnp.float32) / D
    scales = 0.1 * 10.0 ** (0.5 * position + 0.5 * jax.random.uniform(first_key, (D,), jnp.float32))
    rows = jnp.arange(TOKENS, dtype=jnp.float32) / TOKENS
    rising = 3.0 ** rows
    base = jnp.clip(jax.random.normal(second_key, (TOKENS, D), jnp.float32), -4.0, 4.0)
    return (base * scales[None, :] * rising[:, None]).astype(jnp.bfloat16)


def plant(entries, rng, least, largest):
    dims = entries.shape
    spot = [jax.random.randint(jax.random.fold_in(rng, axis), (), 0, dims[axis]) for axis in range(len(dims))]
    entries = entries.at[tuple(spot)].set(least)
    longest = dims.index(max(dims))
    spot[longest] = (spot[longest] + 1) % dims[longest]
    return entries.at[tuple(spot)].set(largest)


def levels(own_key, extent, shards, least, high):
    gain = 1.0
    for axis_at, blocks in shards:
        steps = jax.random.uniform(jax.random.fold_in(jax.random.fold_in(own_key, 6), axis_at), (blocks,), jnp.float32, least / len(shards), high / len(shards))
        gain = gain * jnp.repeat(jnp.exp(steps), extent[axis_at] // blocks).reshape((-1,) + (1,) * (len(extent) - 1 - axis_at))
    return gain


def centred(own_key, extent, spread, reach, cuts=(), kind=jnp.bfloat16):
    array = jax.random.normal(own_key, extent, jnp.float32) * spread
    if len(cuts) > 0:
        array = levels(own_key, extent, cuts, -0.22, 0.18) * array
    return jnp.clip(array, min=-reach, max=reach).astype(kind)


def setup_inputs(seed: int = 0) -> dict:
    key_of = jax.random.split(jax.random.key(seed), 15)
    tokens = draw_tokens(jax.random.fold_in(key_of[14], 71), 0)
    target = centred(key_of[1], (TOKENS, D), 1.0, 6.0, ((0, 16), (1, 16)))
    gate_weight = centred(key_of[2], (D, FF), D ** -0.5, 0.09375, ((0, 16), (1, 16)))
    up_weight = centred(key_of[3], (D, FF), D ** -0.5, 0.09375, ((0, 16), (1, 16)))
    down_weight = centred(key_of[4], (FF, D), FF ** -0.5, 0.078125, ((0, 16), (1, 16)))
    probe_gate = plant(jax.random.randint(key_of[5], (D, FF), 0, 2), jax.random.fold_in(key_of[5], 1), 0, 1).astype(jnp.int32)
    probe_up = plant(jax.random.randint(key_of[6], (D, FF), 0, 2), jax.random.fold_in(key_of[6], 1), 0, 1).astype(jnp.int32)
    probe_down = plant(jax.random.randint(key_of[7], (FF, D), 0, 2), jax.random.fold_in(key_of[7], 1), 0, 1).astype(jnp.int32)
    first_gate = centred(key_of[8], (D, FF), 0.3, 1.8, ((0, 16), (1, 16)), jnp.float32)
    first_up = centred(key_of[9], (D, FF), 0.3, 1.8, ((0, 16), (1, 16)), jnp.float32)
    first_down = centred(key_of[10], (FF, D), 0.3, 1.8, ((0, 16), (1, 16)), jnp.float32)
    second_gate = jnp.clip(jnp.exp(math.log(0.2) - 2.9957323 * jax.random.uniform(key_of[11], (D, FF), jnp.float32) ** levels(key_of[11], (D, FF), ((0, 16), (1, 16)), -0.2, 0.2)), 0.01, 0.2)
    second_up = jnp.clip(jnp.exp(math.log(0.2) - 2.9957323 * jax.random.uniform(key_of[12], (D, FF), jnp.float32) ** levels(key_of[12], (D, FF), ((0, 16), (1, 16)), -0.2, 0.2)), 0.01, 0.2)
    second_down = jnp.clip(jnp.exp(math.log(0.2) - 2.9957323 * jax.random.uniform(key_of[13], (FF, D), jnp.float32) ** levels(key_of[13], (FF, D), ((0, 16), (1, 16)), -0.2, 0.2)), 0.01, 0.2)
    return {"tokens": tokens, "target": target, "gate_weight": gate_weight, "up_weight": up_weight, "down_weight": down_weight, "probe_gate": probe_gate, "probe_up": probe_up, "probe_down": probe_down, "first_gate": first_gate, "first_up": first_up, "first_down": first_down, "second_gate": second_gate, "second_up": second_up, "second_down": second_down}


def activation(pre):
    sig = jax.nn.sigmoid(pre)
    act = pre * sig
    slope = sig * (1.0 + pre * (1.0 - sig))
    bend = sig * (1.0 - sig) * (2.0 + pre * (1.0 - 2.0 * sig))
    return (act, slope, bend)

def block_mean(values):
    height, breadth = values.shape
    means = values.reshape(height // 4, 4, breadth // 4, 4).mean(axis=(1, 3))
    return jnp.broadcast_to(means[:, None, :, None], (height // 4, 4, breadth // 4, 4)).reshape(height, breadth)

def matmul(left, right):
    return jnp.dot(left, right, preferred_element_type=jnp.float32)

def rounded_runs(term_of, pieces):
    total = None
    for index in range(pieces):
        part = term_of(index)
        part = jax.tree.map(lambda value: lax.optimization_barrier(value.astype(jnp.bfloat16)).astype(jnp.float32), part)
        total = part if total is None else jax.tree.map(lambda first, second: first + second, total, part)
    return total

def reference(tokens, target, gate_weight, up_weight, down_weight, probe_gate, probe_up, probe_down, first_gate, first_up, first_down, second_gate, second_up, second_down):
    sign_gate = (2 * probe_gate - 1).astype(jnp.bfloat16)
    sign_up = (2 * probe_up - 1).astype(jnp.bfloat16)
    sign_down = (2 * probe_down - 1).astype(jnp.bfloat16)
    feat_run = D // N_ROW
    unit_run = FF // N_COL

    def project(index):
        lower = index * feat_run
        block = tokens[:, lower:lower + feat_run]
        return (matmul(block, gate_weight[lower:lower + feat_run]), matmul(block, up_weight[lower:lower + feat_run]), matmul(block, sign_gate[lower:lower + feat_run]), matmul(block, sign_up[lower:lower + feat_run]))
    pre_gate, pre_up, dot_gate, dot_up = rounded_runs(project, N_ROW)
    act, slope, bend = activation(pre_gate)
    hidden = (act * pre_up).astype(jnp.bfloat16)
    hidden_dot = (slope * dot_gate * pre_up + act * dot_up).astype(jnp.bfloat16)

    def forward(index):
        lower = index * unit_run
        plain = hidden[:, lower:lower + unit_run]
        tangent = hidden_dot[:, lower:lower + unit_run]
        weight = down_weight[lower:lower + unit_run]
        return (matmul(plain, weight), matmul(tangent, weight) + matmul(plain, sign_down[lower:lower + unit_run]))
    out_val, out_dot = rounded_runs(forward, N_COL)
    err = (out_val - target.astype(jnp.float32)).astype(jnp.bfloat16)
    err_dot = out_dot.astype(jnp.bfloat16)

    def backward(index):
        lower = index * feat_run
        err_part = err[:, lower:lower + feat_run]
        dot_part = err_dot[:, lower:lower + feat_run]
        weight = down_weight[:, lower:lower + feat_run]
        return (matmul(err_part, weight.T), matmul(dot_part, weight.T) + matmul(err_part, sign_down[:, lower:lower + feat_run].T))
    d_hidden, d_hidden_dot = rounded_runs(backward, N_ROW)
    grad_down = matmul(hidden.T, err)
    hess_down = matmul(hidden_dot.T, err) + matmul(hidden.T, err_dot)
    d_gate = (d_hidden * pre_up * slope).astype(jnp.bfloat16)
    d_up = (d_hidden * act).astype(jnp.bfloat16)
    dd_gate = (d_hidden_dot * pre_up * slope + d_hidden * dot_up * slope + d_hidden * pre_up * bend * dot_gate).astype(jnp.bfloat16)
    dd_up = (d_hidden_dot * act + d_hidden * slope * dot_gate).astype(jnp.bfloat16)
    grad_gate = matmul(tokens.T, d_gate)
    grad_up = matmul(tokens.T, d_up)
    hess_gate = matmul(tokens.T, dd_gate)
    hess_up = matmul(tokens.T, dd_up)
    curv_gate = block_mean(jnp.abs(sign_gate.astype(jnp.float32) * hess_gate))
    curv_up = block_mean(jnp.abs(sign_up.astype(jnp.float32) * hess_up))
    curv_down = block_mean(jnp.abs(sign_down.astype(jnp.float32) * hess_down))
    count = 3.0 * D * FF
    total_grad = jnp.sum(grad_gate * grad_gate) + jnp.sum(grad_up * grad_up) + jnp.sum(grad_down * grad_down)
    total_curv = jnp.sum(curv_gate * curv_gate) + jnp.sum(curv_up * curv_up) + jnp.sum(curv_down * curv_down)
    rms_grad = jnp.sqrt(total_grad / count + 1e-06)
    rms_curv = jnp.sqrt(total_curv / count + 1e-06)
    fix_first = 1.0 - 0.9 ** STEP
    fix_second = 1.0 - 0.95 ** STEP
    firsts = []
    seconds = []
    updates = []
    for grad, curv, first, second in ((grad_gate, curv_gate, first_gate, second_gate), (grad_up, curv_up, first_up, second_up), (grad_down, curv_down, first_down, second_down)):
        new_first = 0.9 * first + 0.1 * (grad / rms_grad)
        scaled = curv / rms_curv
        new_second = 0.95 * second + 0.05 * (scaled * scaled)
        firsts.append(new_first)
        seconds.append(new_second)
        updates.append(new_first / fix_first / (jnp.sqrt(new_second / fix_second) + 1e-08))
    return (firsts[0], firsts[1], firsts[2], seconds[0], seconds[1], seconds[2], updates[0], updates[1], updates[2])
```

```python
import functools

import jax
import jax.numpy as jnp
from jax import lax
from jax.experimental import pallas as pl
from jax.experimental.pallas import tpu as pltpu
from jax.sharding import Mesh
from jax.sharding import PartitionSpec as P

D = 4096
FF = 5504
STEP = 10
COL = ("col_0", "col_1")
ROW = ("row_0", "row_1", "row_2")
ROW_COL = ("row_0", "row_1", "row_2", "col_0", "col_1")


def copy_for_each(shard, axis):
    length = lax.axis_size(axis)
    return lax.all_to_all(
        jnp.broadcast_to(shard[None], (length, *shard.shape)), axis, 0, 0, tiled=True
    )


def laid_out(parts, dim):
    parts = jnp.moveaxis(parts, 0, dim)
    dims = parts.shape
    return parts.reshape(*dims[:dim], dims[dim] * dims[dim + 1], *dims[dim + 2 :])


def collect(shard, axis, dim):
    parts = copy_for_each(shard, axis)
    return laid_out(parts, dim)


def split_up(shard, dim, length):
    dims = shard.shape
    parts = shard.reshape(*dims[:dim], length, dims[dim] // length, *dims[dim + 1 :])
    return jnp.moveaxis(parts, dim, 0)


def sent_and_summed(shard, axis, dim):
    length = lax.axis_size(axis)
    parts = lax.all_to_all(split_up(shard, dim, length), axis, 0, 0, tiled=True)
    return jnp.sum(parts.astype(jnp.float32), axis=0)


def over_axes(shard, axes):
    return functools.reduce(lax.psum, axes, shard)


def activation(pre):
    sig = jax.nn.sigmoid(pre)
    act = pre * sig
    slope = sig * (1.0 + pre * (1.0 - sig))
    bend = sig * (1.0 - sig) * (2.0 + pre * (1.0 - 2.0 * sig))
    return (act, slope, bend)


def block_ones(size):
    rows = lax.broadcasted_iota(jnp.int32, (size, size), 0) >> 2
    cols = lax.broadcasted_iota(jnp.int32, (size, size), 1) >> 2
    return (rows == cols).astype(jnp.float32)


def exact_dot(left, right):
    return jnp.dot(
        left, right, preferred_element_type=jnp.float32, precision=lax.Precision.HIGHEST
    )


def curvature(sign, hess):
    height, breadth = hess.shape
    down = exact_dot(block_ones(height), jnp.abs(sign * hess))
    return exact_dot(down, block_ones(breadth)) * 0.0625


def tail_kernel(*refs):
    hess_refs, sign_refs, grad_refs, curv_refs, sums_ref = (
        refs[0:3],
        refs[3:6],
        refs[6:9],
        refs[9:12],
        refs[12],
    )
    grad_sum = 0.0
    curv_sum = 0.0
    for hess_ref, sign_ref, grad_ref, curv_ref in zip(hess_refs, sign_refs, grad_refs, curv_refs):
        sign = (2 * sign_ref[...] - 1).astype(jnp.float32)
        curv = curvature(sign, hess_ref[...])
        curv_ref[...] = curv
        grad = grad_ref[...]
        grad_sum = grad_sum + jnp.sum(grad * grad, axis=(0, 1), keepdims=True)
        curv_sum = curv_sum + jnp.sum(curv * curv, axis=(0, 1), keepdims=True)
    lane = lax.broadcasted_iota(jnp.int32, (1, 128), 1)
    sums_ref[...] = jnp.where(lane == 0, grad_sum, jnp.where(lane == 1, curv_sum, 0.0))


def matmul(left, right):
    return jnp.dot(left, right, preferred_element_type=jnp.float32)


def inner_first(left, right):
    return lax.dot_general(
        left, right, (((0,), (0,)), ((), ())), preferred_element_type=jnp.float32
    )


def inner_last(left, right):
    return lax.dot_general(
        left, right, (((1,), (1,)), ((), ())), preferred_element_type=jnp.float32
    )


def body(
    tokens,
    target,
    gate_weight,
    up_weight,
    down_weight,
    probe_gate,
    probe_up,
    probe_down,
    first_gate,
    first_up,
    first_down,
    second_gate,
    second_up,
    second_down,
):
    whole = collect(tokens, COL, 0)
    sign_gate = (2 * probe_gate - 1).astype(jnp.bfloat16)
    sign_up = (2 * probe_up - 1).astype(jnp.bfloat16)
    sign_down = (2 * probe_down - 1).astype(jnp.bfloat16)
    width = gate_weight.shape[1]

    def projector(matrices):
        return jnp.concatenate([matmul(whole, matrix) for matrix in matrices], axis=1)

    sums = sent_and_summed(projector((gate_weight, up_weight)).astype(jnp.bfloat16), ROW, 0)
    pre_gate = sums[:, :width]
    pre_up = sums[:, width:]
    act, slope, bend = activation(pre_gate)
    hidden = (act * pre_up).astype(jnp.bfloat16)
    moved = sent_and_summed(projector((sign_gate, sign_up)).astype(jnp.bfloat16), ROW, 0)
    dot_gate = moved[:, :width]
    dot_up = moved[:, width:]
    hidden_dot = (slope * dot_gate * pre_up + act * dot_up).astype(jnp.bfloat16)
    both = jnp.concatenate([hidden, hidden_dot], axis=1)
    piece = lax.all_gather(both, ROW, axis=0, tiled=True)
    plain = piece[:, :width]
    tangent = piece[:, width:]
    value = matmul(plain, down_weight)
    along = matmul(tangent, down_weight) + matmul(plain, sign_down)
    terms = jnp.concatenate([value, along], axis=1)
    outputs = sent_and_summed(terms.astype(jnp.bfloat16), COL, 0)
    feats_here = down_weight.shape[1]
    resid = outputs[:, :feats_here] - target.astype(jnp.float32)
    errors = jnp.concatenate(
        [resid.astype(jnp.bfloat16), outputs[:, feats_here:].astype(jnp.bfloat16)], axis=1
    )
    err_all = lax.all_gather(errors, COL, axis=0, tiled=True)
    block = err_all
    err = block[:, :feats_here]
    err_dot = block[:, feats_here:]
    plain = inner_last(err, down_weight)
    along = inner_last(err_dot, down_weight) + inner_last(err, sign_down)
    back = sent_and_summed(jnp.concatenate([plain, along], axis=1).astype(jnp.bfloat16), ROW, 0)
    d_hidden = back[:, :width]
    d_hidden_dot = back[:, width:]
    block = err_all
    piece = lax.all_gather(both, ROW, axis=0, tiled=True)
    plain = piece[:, :width]
    tangent = piece[:, width:]
    err = block[:, :feats_here]
    err_dot = block[:, feats_here:]
    grad_part = inner_first(plain, err)
    hess_part = inner_first(tangent, err) + inner_first(plain, err_dot)
    d_gate = (d_hidden * pre_up * slope).astype(jnp.bfloat16)
    d_up = (d_hidden * act).astype(jnp.bfloat16)
    dd_gate = (
        d_hidden_dot * pre_up * slope
        + d_hidden * dot_up * slope
        + d_hidden * pre_up * bend * dot_gate
    ).astype(jnp.bfloat16)
    dd_up = (d_hidden_dot * act + d_hidden * slope * dot_gate).astype(jnp.bfloat16)
    stacked = jnp.concatenate([d_gate, d_up, dd_gate, dd_up], axis=1)
    block = whole
    grads = inner_first(block, lax.all_gather(stacked, ROW, axis=0, tiled=True))
    grad_gate = grads[:, :width]
    grad_up = grads[:, width : 2 * width]
    hess_gate = grads[:, 2 * width : 3 * width]
    hess_up = grads[:, 3 * width :]
    shapes = [jax.ShapeDtypeStruct(probe.shape, jnp.float32) for probe in (probe_gate, probe_up, probe_down)]
    curv_gate, curv_up, curv_down, sums = pl.pallas_call(
        tail_kernel,
        out_shape=(*shapes, jax.ShapeDtypeStruct((1, 128), jnp.float32)),
        in_specs=[pl.BlockSpec(memory_space=pltpu.VMEM)] * 9,
        out_specs=[pl.BlockSpec(memory_space=pltpu.VMEM)] * 4,
        compiler_params=pltpu.CompilerParams(vmem_limit_bytes=40 * 1024 * 1024),
    )(hess_gate, hess_up, hess_part, probe_gate, probe_up, probe_down, grad_gate, grad_up, grad_part)
    totals = lax.psum(sums[0, :2], ROW_COL)
    total_grad, total_curv = totals[0], totals[1]
    count = 3.0 * D * FF
    rms_grad = jnp.sqrt(total_grad / count + 1e-06)
    rms_curv = jnp.sqrt(total_curv / count + 1e-06)
    fix_first = 1.0 - 0.9**STEP
    fix_second = 1.0 - 0.95**STEP
    firsts = []
    seconds = []
    updates = []
    for grad, curv, first, second in (
        (grad_gate, curv_gate, first_gate, second_gate),
        (grad_up, curv_up, first_up, second_up),
        (grad_part, curv_down, first_down, second_down),
    ):
        new_first = 0.9 * first + 0.1 * (grad / rms_grad)
        scaled = curv / rms_curv
        new_second = 0.95 * second + 0.05 * (scaled * scaled)
        firsts.append(new_first)
        seconds.append(new_second)
        updates.append(new_first / fix_first / (jnp.sqrt(new_second / fix_second) + 1e-08))
    return (
        firsts[0],
        firsts[1],
        firsts[2],
        seconds[0],
        seconds[1],
        seconds[2],
        updates[0],
        updates[1],
        updates[2],
    )


def solution(mesh):
    torus = Mesh(mesh.devices.reshape(4, 2, 2, 4, 4), ("row_0", "row_1", "row_2", "col_0", "col_1"))
    in_specs = (
        P(COL, ROW),
        P(COL, ROW),
        P(ROW, COL),
        P(ROW, COL),
        P(COL, ROW),
        P(ROW, COL),
        P(ROW, COL),
        P(COL, ROW),
        P(ROW, COL),
        P(ROW, COL),
        P(COL, ROW),
        P(ROW, COL),
        P(ROW, COL),
        P(COL, ROW),
    )
    out_specs = (
        P(ROW, COL),
        P(ROW, COL),
        P(COL, ROW),
        P(ROW, COL),
        P(ROW, COL),
        P(COL, ROW),
        P(ROW, COL),
        P(ROW, COL),
        P(COL, ROW),
    )
    return jax.shard_map(body, mesh=torus, in_specs=in_specs, out_specs=out_specs, check_vma=False)
```

```python
import jax
import jax.numpy as jnp
from jax import lax
from jax.experimental import pallas as pl
from jax.experimental.pallas import tpu as pltpu
from jax.sharding import Mesh
from jax.sharding import PartitionSpec as P

D = 4096
FF = 5504
STEP = 10
COL = ("col_0", "col_1")
ROW = ("row_0", "row_1", "row_2")
RING = 4
UNITS = 344
PADDED = 352
FEATS = 256
HALF = 64
LANES = 128
STRIP = 32
MESH = pl.DeviceIdType.MESH
BF16 = jnp.bfloat16
F32 = jnp.float32

X_AXIS, Z_AXIS, CORE_AXIS = ROW
H_AXIS, Y_AXIS = COL


def dot_nn(left, right):
    return jnp.dot(left, right, preferred_element_type=F32)


def dot_nt(left, right):
    return lax.dot_general(left, right, (((1,), (1,)), ((), ())), preferred_element_type=F32)


def dot_tn(left, right):
    return lax.dot_general(left, right, (((0,), (0,)), ((), ())), preferred_element_type=F32)


def block_ones(size):
    rows = lax.broadcasted_iota(jnp.int32, (size, size), 0) >> 2
    cols = lax.broadcasted_iota(jnp.int32, (size, size), 1) >> 2
    return jnp.where(rows == cols, 1.0, 0.0).astype(BF16)


def two_terms(values):
    high = values.astype(BF16)
    low = (values - high.astype(F32)).astype(BF16)
    return high, low


def curvature(sign, hess):
    high, low = two_terms(jnp.abs(sign * hess))
    ones = block_ones(hess.shape[0])
    down = dot_nn(ones, high) + dot_nn(ones, low)
    high, low = two_terms(down)
    ones = block_ones(hess.shape[1])
    return (dot_nn(high, ones) + dot_nn(low, ones)) * 0.0625


class Copies:
    def __init__(self, send_sems, recv_sems):
        self.send_sems = send_sems
        self.recv_sems = recv_sems
        self.next = 0
        self.pending = []

    def slots(self, count):
        first = self.next
        self.next += count
        return first

    def copy(self, src, dst, slot, peer):
        return pltpu.make_async_remote_copy(
            src_ref=src,
            dst_ref=dst,
            send_sem=self.send_sems.at[slot],
            recv_sem=self.recv_sems.at[slot],
            device_id=peer,
            device_id_type=MESH,
        )

    def send(self, src, dst, slot, peer):
        self.copy(src, dst, slot, peer).start()

    def arrived(self, dst, slot, peer):
        self.copy(dst, dst, slot, peer).wait_recv()

    def sent(self, src, slot, peer):
        self.copy(src, src, slot, peer).wait_send()


def around(axis):
    here = lax.axis_index(axis)
    return here, lax.rem(here + 1, RING), lax.rem(here + 3, RING), lax.rem(here + 2, RING)


def add_strips(dst, terms):
    def strip(index, carry):
        rows = pl.ds(pl.multiple_of(index * STRIP, STRIP), STRIP)
        total = terms[0][rows, :].astype(F32)
        for term in terms[1:]:
            total = total + term[rows, :].astype(F32)
        dst[rows, :] = total.astype(dst.dtype)
        return carry

    lax.fori_loop(0, PADDED // STRIP, strip, 0)


def add_blocks(dst, terms):
    for part in range(2):
        total = terms[0][part].astype(F32)
        for term in terms[1:]:
            total = total + term[part].astype(F32)
        dst[part] = total.astype(dst.dtype)


class RingSum:
    def __init__(self, copies, axis, count, block, landed, add):
        self.copies, self.axis, self.block, self.landed, self.add = copies, axis, block, landed, add
        self.base = copies.slots(6 * count)
        self.count = count
        self.here, self.plus, self.minus, self.opposite = around(axis)

    def slot(self, kind, index):
        return self.base + kind * self.count + index

    def send(self, src, kind, index, peer):
        self.copies.send(src, self.landed(kind, index), self.slot(kind, index), {self.axis: peer})

    def wait(self, kind, index):
        ref = self.landed(kind, index)
        self.copies.arrived(ref, self.slot(kind, index), {self.axis: self.plus})

    def send_opposite(self, index):
        self.send(self.block(self.opposite, 0, index), 0, index, self.plus)
        self.send(self.block(self.opposite, 1, index), 1, index, self.minus)

    def send_plus(self, index):
        self.send(self.block(self.plus, 1, index), 3, index, self.plus)

    def send_minus(self, index):
        self.send(self.block(self.minus, 0, index), 4, index, self.minus)

    def forward(self, index):
        self.wait(0, index)
        ref = self.block(self.plus, 0, index)
        self.add(ref, (ref, self.landed(0, index)))
        self.send(ref, 2, index, self.plus)
        self.wait(1, index)
        ref = self.block(self.minus, 1, index)
        self.add(ref, (ref, self.landed(1, index)))
        self.send(ref, 5, index, self.minus)

    def wait_terms(self, index):
        for kind in (3, 4, 2, 5):
            self.wait(kind, index)

    def terms(self, half, index):
        return (
            self.block(self.here, half, index),
            self.landed(2 + half, index),
            self.landed(4 + half, index),
        )

    def drain(self, index):
        for kind in range(6):
            self.copies.sent(
                self.landed(kind, index), self.slot(kind, index), {self.axis: self.plus}
            )


class RowSum:
    def __init__(self, copies, count, blocks, landed, pair_sums, pair_landed):
        self.copies, self.count = copies, count
        self.ring = RingSum(
            copies,
            X_AXIS,
            count,
            lambda place, half, index: blocks.at[place, half, index],
            lambda kind, index: landed.at[kind, index],
            add_strips,
        )
        self.base = copies.slots(count)
        self.pair_sums, self.pair_landed = pair_sums, pair_landed
        self.z = lax.axis_index(Z_AXIS)
        self.other = 1 - self.z

    def pair(self, index):
        self.ring.wait_terms(index)
        add_strips(self.pair_sums.at[index], self.ring.terms(self.other, index))
        self.copies.send(
            self.pair_sums.at[index],
            self.pair_landed.at[index],
            self.base + index,
            {Z_AXIS: self.other},
        )

    def finish(self, dst, index):
        self.copies.arrived(self.pair_landed.at[index], self.base + index, {Z_AXIS: self.other})
        add_strips(dst, (*self.ring.terms(self.z, index), self.pair_landed.at[index]))

    def drain(self, index):
        self.ring.drain(index)
        self.copies.sent(self.pair_sums.at[index], self.base + index, {Z_AXIS: self.other})


class RowGather:
    def __init__(self, copies, count, buffer):
        self.copies, self.count, self.buffer = copies, count, buffer
        self.base = copies.slots(7 * count)
        self.here, self.plus, self.minus, self.opposite = around(X_AXIS)
        self.z = lax.axis_index(Z_AXIS)
        self.other = 1 - self.z

    def send(self, place, z, kind, index, peer):
        ref = self.buffer.at[place, z, index]
        self.copies.send(ref, ref, self.base + kind * self.count + index, peer)

    def wait(self, place, z, kind, index):
        ref = self.buffer.at[place, z, index]
        slot = self.base + kind * self.count + index
        self.copies.arrived(ref, slot, {Z_AXIS: self.other})

    def start(self, index):
        self.send(self.here, self.z, 0, index, {Z_AXIS: self.other})
        self.send(self.here, self.z, 1, index, {X_AXIS: self.plus})
        self.send(self.here, self.z, 2, index, {X_AXIS: self.minus})

    def pair(self, index):
        self.wait(self.here, self.other, 0, index)
        self.send(self.here, self.other, 3, index, {X_AXIS: self.plus})
        self.send(self.here, self.other, 4, index, {X_AXIS: self.minus})

    def forward(self, index):
        self.wait(self.minus, self.z, 1, index)
        self.wait(self.minus, self.other, 3, index)
        self.send(self.minus, 0, 5, index, {X_AXIS: self.plus})
        self.wait(self.plus, self.z, 2, index)
        self.wait(self.plus, self.other, 4, index)
        self.send(self.plus, 1, 6, index, {X_AXIS: self.minus})

    def finish(self, index):
        self.wait(self.opposite, 0, 5, index)
        self.wait(self.opposite, 1, 6, index)

    def drain(self, index):
        for kind in range(7):
            ref = self.buffer.at[0, 0, index]
            slot = self.base + kind * self.count + index
            self.copies.sent(ref, slot, {Z_AXIS: self.other})


class RingGather:
    def __init__(self, copies, axis, whole, half):
        self.copies, self.axis, self.whole, self.half = copies, axis, whole, half
        self.base = copies.slots(4)
        self.here, self.plus, self.minus, self.opposite = around(axis)

    def send(self, ref, kind, peer):
        self.copies.send(ref, ref, self.base + kind, {self.axis: peer})

    def wait(self, ref, kind):
        self.copies.arrived(ref, self.base + kind, {self.axis: self.plus})

    def start(self):
        self.send(self.whole(self.here), 0, self.plus)
        self.send(self.whole(self.here), 1, self.minus)

    def from_minus(self):
        self.wait(self.whole(self.minus), 0)
        self.send(self.half(self.minus, 0), 2, self.plus)

    def from_plus(self):
        self.wait(self.whole(self.plus), 1)
        self.send(self.half(self.plus, 1), 3, self.minus)

    def finish(self):
        self.wait(self.half(self.opposite, 0), 2)
        self.wait(self.half(self.opposite, 1), 3)

    def drain(self):
        for kind in range(4):
            ref = self.whole(0) if kind < 2 else self.half(0, 0)
            self.copies.sent(ref, self.base + kind, {self.axis: self.plus})


class ColGather:
    def __init__(self, copies, buffer):
        here, plus, minus, opposite = around(H_AXIS)
        y = lax.axis_index(Y_AXIS)
        self.outer = RingGather(
            copies,
            H_AXIS,
            lambda place: buffer.at[place, y],
            lambda place, half: buffer.at[place, y, half],
        )
        self.inner = [
            RingGather(
                copies,
                Y_AXIS,
                lambda place, layer=layer: buffer.at[layer, place],
                lambda place, half, layer=layer: buffer.at[layer, place, half],
            )
            for layer in (here, minus, plus, opposite)
        ]

    def start(self):
        self.outer.start()
        self.inner[0].start()

    def run(self):
        self.outer.from_minus()
        self.inner[1].start()
        self.outer.from_plus()
        self.inner[2].start()
        self.inner[0].from_minus()
        self.inner[0].from_plus()
        self.outer.finish()
        self.inner[3].start()
        for inner in self.inner[1:]:
            inner.from_minus()
            inner.from_plus()
        for inner in self.inner:
            inner.finish()

    def drain(self):
        self.outer.drain()
        for inner in self.inner:
            inner.drain()


def step_kernel(
    tokens,
    target,
    gate_weight,
    up_weight,
    down_weight,
    probe_gate,
    probe_up,
    probe_down,
    grad_gate_out,
    grad_up_out,
    grad_down_out,
    curv_gate_out,
    curv_up_out,
    curv_down_out,
    sums_out,
    wide,
    tall,
    proj,
    down,
    x,
    tgt,
    part,
    part_landed,
    pair_sums,
    pair_landed,
    pre,
    hid,
    outs,
    outs_landed,
    layer_sums,
    layer_landed,
    final,
    err,
    back,
    back_landed,
    back_pair,
    back_pair_landed,
    d_hid,
    d_pre,
    grads,
    grads_landed,
    grads_down,
    grads_down_landed,
    tiles,
    tiles_landed,
    send_sems,
    recv_sems,
):
    copies = Copies(send_sems, recv_sems)
    core = lax.axis_index(CORE_AXIS)
    other_core = 1 - core
    x_here, x_plus, x_minus, x_opposite = around(X_AXIS)
    y_here, y_plus, y_minus, y_opposite = around(Y_AXIS)
    h_here, h_plus, h_minus, h_opposite = around(H_AXIS)
    z_here = lax.axis_index(Z_AXIS)
    partner = {CORE_AXIS: other_core}

    barrier = pltpu.get_barrier_semaphore()
    peers = [partner, {Z_AXIS: 1 - z_here}]
    for axis in (X_AXIS, Y_AXIS, H_AXIS):
        peers += [{axis: place} for place in around(axis)[1:]]
    for peer in peers:
        pl.semaphore_signal(barrier, inc=1, device_id=peer, device_id_type=MESH)

    own_rows = pl.ds(pl.multiple_of(core * HALF, HALF), HALF)
    other_rows = pl.ds(pl.multiple_of(other_core * HALF, HALF), HALF)
    x[h_here, y_here, core] = tokens[own_rows, :]
    tgt[core] = target[own_rows, :]

    def lay_out(source, index):
        wide[:, FEATS:] = jnp.zeros((FEATS, 3 * LANES - FEATS), BF16)
        wide[:, :UNITS] = source
        proj[core, index] = wide[...].T[:PADDED]

    def sign(ref):
        return (2 * ref[...] - 1).astype(F32).astype(BF16)

    lay_out(gate_weight[...], 0)
    lay_out(up_weight[...], 1)
    lay_out(sign(probe_gate), 2)
    lay_out(sign(probe_up), 3)
    rest = jnp.zeros((32, FEATS), BF16)
    down[core, 0, PADDED - 32 :] = rest
    down[core, 1, PADDED - 32 :] = rest
    down[core, 0, :UNITS] = down_weight[...]
    down[core, 1, :UNITS] = sign(probe_down)

    pl.semaphore_wait(barrier, len(peers))
    near = copies.slots(6)
    copies.send(tokens.at[other_rows], x.at[h_here, y_here, core], near, partner)
    copies.send(proj.at[core], proj.at[core], near + 1, partner)
    copies.send(target.at[other_rows], tgt.at[core], near + 2, partner)
    copies.send(down.at[core], down.at[core], near + 3, partner)

    copies.arrived(x.at[h_here, y_here, other_core], near, partner)
    x_gather = ColGather(copies, x)
    x_gather.start()
    x_gather.run()
    copies.arrived(proj.at[other_core], near + 1, partner)

    def token_block(ref, place, *rest):
        return [
            ref[(place, slice(None), *rest, half)].reshape(RING * HALF, FEATS) for half in range(2)
        ]

    row_sum = RowSum(copies, 4, part, part_landed, pair_sums, pair_landed)

    def project(index, place):
        left, right = token_block(x, place)
        both = dot_nt(proj[0, index], left) + dot_nt(proj[1, index], right)
        both = both.astype(BF16)
        part[place, 0, index] = both[:, :LANES]
        part[place, 1, index] = both[:, LANES:]

    def project_all(index, carry):
        project(index, x_opposite)
        row_sum.ring.send_opposite(index)
        project(index, x_plus)
        row_sum.ring.send_plus(index)
        project(index, x_minus)
        row_sum.ring.send_minus(index)
        project(index, x_here)
        return carry

    def each(count, step):
        def body(index, carry):
            step(index)
            return carry

        lax.fori_loop(0, count, body, 0)

    lax.fori_loop(0, 4, project_all, 0)
    each(4, row_sum.ring.forward)
    each(4, row_sum.pair)
    each(4, lambda index: row_sum.finish(pre.at[index], index))

    def strips(step):
        def body(index, carry):
            step(pl.ds(pl.multiple_of(index * STRIP, STRIP), STRIP))
            return carry

        lax.fori_loop(0, PADDED // STRIP, body, 0)

    def hide(rows):
        pre_gate, pre_up = pre[0, rows, :], pre[1, rows, :]
        dot_gate, dot_up = pre[2, rows, :], pre[3, rows, :]
        sig = jax.nn.sigmoid(pre_gate)
        act = pre_gate * sig
        slope = sig * (1.0 + pre_gate * (1.0 - sig))
        hid[x_here, z_here, 0, rows, :] = (act * pre_up).astype(BF16)
        hid[x_here, z_here, 1, rows, :] = (slope * dot_gate * pre_up + act * dot_up).astype(BF16)

    strips(hide)
    hid_gather = RowGather(copies, 2, hid)
    each(2, hid_gather.start)
    each(2, hid_gather.pair)
    copies.arrived(down.at[other_core], near + 3, partner)

    out_sum = RingSum(
        copies,
        Y_AXIS,
        4,
        lambda place, half, layer: outs.at[layer[1], place, half],
        lambda kind, layer: outs_landed.at[kind, layer[0]],
        add_blocks,
    )
    out_sum.slot = lambda kind, layer: out_sum.base + kind * 4 + layer[0]

    def whole_units(ref, place, index):
        return jnp.concatenate([ref[place, 0, index], ref[place, 1, index]], axis=1)

    def expand(place):
        plain = whole_units(hid, place, 0)
        tangent = whole_units(hid, place, 1)
        for half in range(2):
            value = dot_tn(plain, down[half, 0])
            along = dot_tn(tangent, down[half, 0]) + dot_tn(plain, down[half, 1])
            value = value.astype(BF16).reshape(RING, HALF, FEATS)
            along = along.astype(BF16).reshape(RING, HALF, FEATS)
            for block in range(RING):
                outs[place, block, 0, half] = value[block]
                outs[place, block, 1, half] = along[block]

    layers = [(0, x_here), (1, x_minus), (2, x_plus), (3, x_opposite)]

    def expand_and_send(layer):
        expand(layer[1])
        out_sum.send_opposite(layer)
        out_sum.send_plus(layer)
        out_sum.send_minus(layer)

    expand_and_send(layers[0])
    each(2, hid_gather.forward)
    expand_and_send(layers[1])
    expand_and_send(layers[2])
    out_sum.forward(layers[0])
    each(2, hid_gather.finish)
    expand_and_send(layers[3])
    for layer in layers[1:]:
        out_sum.forward(layer)
    for layer in layers:
        out_sum.wait_terms(layer)
        for half in range(2):
            add_blocks(layer_sums.at[layer[1], half], out_sum.terms(half, layer))

    layer_sum = RingSum(
        copies,
        H_AXIS,
        1,
        lambda place, half, index: layer_sums.at[place, half],
        lambda kind, index: layer_landed.at[kind],
        add_blocks,
    )
    layer_sum.send_opposite(0)
    layer_sum.send_plus(0)
    layer_sum.send_minus(0)
    layer_sum.forward(0)
    layer_sum.wait_terms(0)
    copies.arrived(tgt.at[other_core], near + 2, partner)
    for half in range(2):
        add_blocks(final.at[half], layer_sum.terms(half, 0))
    for side in range(2):
        value = final[0, side] - tgt[side].astype(F32)
        err[h_here, y_here, 0, side] = value.astype(BF16)
        err[h_here, y_here, 1, side] = final[1, side].astype(BF16)

    err_gather = ColGather(copies, err)
    err_gather.start()
    err_gather.run()

    back_sum = RowSum(copies, 2, back, back_landed, back_pair, back_pair_landed)

    def turn_back(place):
        plain = token_block(err, place, 0)
        tangent = token_block(err, place, 1)
        value = dot_nt(down[0, 0], plain[0]) + dot_nt(down[1, 0], plain[1])
        along = dot_nt(down[0, 0], tangent[0]) + dot_nt(down[1, 0], tangent[1])
        along = along + dot_nt(down[0, 1], plain[0]) + dot_nt(down[1, 1], plain[1])
        for index, whole in enumerate((value, along)):
            whole = whole.astype(BF16)
            back[place, 0, index] = whole[:, :LANES]
            back[place, 1, index] = whole[:, LANES:]

    turn_back(x_opposite)
    each(2, back_sum.ring.send_opposite)
    turn_back(x_plus)
    each(2, back_sum.ring.send_plus)
    turn_back(x_minus)
    each(2, back_sum.ring.send_minus)
    turn_back(x_here)
    each(2, back_sum.ring.forward)
    each(2, back_sum.pair)
    each(2, lambda index: back_sum.finish(d_hid.at[index], index))

    def slopes(rows):
        pre_gate, pre_up = pre[0, rows, :], pre[1, rows, :]
        dot_gate, dot_up = pre[2, rows, :], pre[3, rows, :]
        d_hidden, d_hidden_dot = d_hid[0, rows, :], d_hid[1, rows, :]
        sig = jax.nn.sigmoid(pre_gate)
        act = pre_gate * sig
        slope = sig * (1.0 + pre_gate * (1.0 - sig))
        bend = sig * (1.0 - sig) * (2.0 + pre_gate * (1.0 - 2.0 * sig))
        dd_gate = (
            d_hidden_dot * pre_up * slope
            + d_hidden * dot_up * slope
            + d_hidden * pre_up * bend * dot_gate
        )
        dd_up = d_hidden_dot * act + d_hidden * slope * dot_gate
        d_pre[x_here, z_here, 0, rows, :] = (d_hidden * pre_up * slope).astype(BF16)
        d_pre[x_here, z_here, 1, rows, :] = (d_hidden * act).astype(BF16)
        d_pre[x_here, z_here, 2, rows, :] = dd_gate.astype(BF16)
        d_pre[x_here, z_here, 3, rows, :] = dd_up.astype(BF16)

    strips(slopes)
    pre_gather = RowGather(copies, 4, d_pre)
    each(4, pre_gather.start)
    each(4, pre_gather.pair)
    each(4, pre_gather.forward)

    def down_grads(side):
        plain_sum = jnp.zeros((PADDED, FEATS), F32)
        along_sum = jnp.zeros((PADDED, FEATS), F32)
        for place in range(RING):
            plain = whole_units(hid, place, 0)
            tangent = whole_units(hid, place, 1)
            err_block = err[place, :, 0, side].reshape(RING * HALF, FEATS)
            dot_block = err[place, :, 1, side].reshape(RING * HALF, FEATS)
            plain_sum = plain_sum + dot_nn(plain, err_block)
            along_sum = along_sum + dot_nn(tangent, err_block) + dot_nn(plain, dot_block)
        grads_down[side, 0] = plain_sum
        grads_down[side, 1] = along_sum

    down_grads(other_core)
    copies.send(grads_down.at[other_core], grads_down_landed, near + 4, partner)
    down_grads(core)

    each(4, pre_gather.finish)

    def pre_grads(side):
        def one(index):
            total = jnp.zeros((PADDED, FEATS), F32)
            for place in range(RING):
                tokens_block = x[place, :, side].reshape(RING * HALF, FEATS)
                total = total + dot_nn(whole_units(d_pre, place, index), tokens_block)
            grads[side, index] = total

        each(4, one)

    pre_grads(other_core)
    copies.send(grads.at[other_core], grads_landed, near + 5, partner)
    pre_grads(core)

    def squares(values):
        return jnp.sum(values * values, axis=0, keepdims=True)

    copies.arrived(grads_down_landed, near + 4, partner)
    grad = grads_down[core, 0] + grads_down_landed[0]
    hess = grads_down[core, 1] + grads_down_landed[1]
    grad_down_out[...] = grad[:UNITS]
    grad_sum = squares(grad)
    curv = curvature(down[core, 1].astype(F32), hess)
    curv_down_out[...] = curv[:UNITS]
    curv_sum = squares(curv)

    tall[PADDED - 32 :] = jnp.zeros((3 * LANES - PADDED + 32, FEATS), F32)

    def turned(values, out):
        tall[:PADDED] = values
        out[...] = tall[...].T[:, :UNITS]

    copies.arrived(grads_landed, near + 5, partner)
    for index, (grad_out, curv_out) in enumerate(
        ((grad_gate_out, curv_gate_out), (grad_up_out, curv_up_out))
    ):
        grad = grads[core, index] + grads_landed[index]
        turned(grad, grad_out)
        grad_sum = grad_sum + squares(grad)
        hess = grads[core, 2 + index] + grads_landed[2 + index]
        curv = curvature(proj[core, 2 + index].astype(F32), hess)
        turned(curv, curv_out)
        curv_sum = curv_sum + squares(curv)

    lane = lax.broadcasted_iota(jnp.int32, (8, LANES), 1)
    grad_sum = jnp.sum(grad_sum, axis=1, keepdims=True)
    curv_sum = jnp.sum(curv_sum, axis=1, keepdims=True)
    tiles[0] = jnp.where(lane == 0, grad_sum, jnp.where(lane == 1, curv_sum, 0.0))

    stages = [
        [partner],
        [{Z_AXIS: 1 - z_here}],
        [{X_AXIS: x_plus}, {X_AXIS: x_opposite}, {X_AXIS: x_minus}],
        [{Y_AXIS: y_plus}, {Y_AXIS: y_opposite}, {Y_AXIS: y_minus}],
        [{H_AXIS: h_plus}, {H_AXIS: h_opposite}, {H_AXIS: h_minus}],
    ]
    small = copies.slots(3 * len(stages))
    for stage, receivers in enumerate(stages):
        for index, peer in enumerate(receivers):
            slot = small + 3 * stage + index
            copies.send(tiles.at[stage], tiles_landed.at[stage, index], slot, peer)
        total = tiles[stage]
        for index, peer in enumerate(receivers):
            copies.arrived(tiles_landed.at[stage, index], small + 3 * stage + index, peer)
            total = total + tiles_landed[stage, index]
        tiles[stage + 1] = total
    sums_out[...] = tiles[len(stages)]

    copies.sent(x.at[0, 0, 0], near, partner)
    copies.sent(proj.at[0], near + 1, partner)
    copies.sent(tgt.at[0], near + 2, partner)
    copies.sent(down.at[0], near + 3, partner)
    copies.sent(grads_down_landed, near + 4, partner)
    copies.sent(grads_landed, near + 5, partner)
    x_gather.drain()
    err_gather.drain()
    each(4, row_sum.drain)
    each(2, back_sum.drain)
    each(2, hid_gather.drain)
    each(4, pre_gather.drain)
    for layer in layers:
        out_sum.drain(layer)
    layer_sum.drain(0)
    for stage, receivers in enumerate(stages):
        for index, peer in enumerate(receivers):
            copies.sent(tiles.at[stage], small + 3 * stage + index, peer)


SLOTS = 240


def whole_step(*operands):
    natural = jax.ShapeDtypeStruct((FEATS, UNITS), F32)
    turned = jax.ShapeDtypeStruct((UNITS, FEATS), F32)
    units = (PADDED, LANES)
    block = (2, HALF, FEATS)
    return pl.pallas_call(
        step_kernel,
        out_shape=(
            natural,
            natural,
            turned,
            natural,
            natural,
            turned,
            jax.ShapeDtypeStruct((8, LANES), F32),
        ),
        in_specs=[pl.BlockSpec(memory_space=pltpu.VMEM)] * 8,
        out_specs=[pl.BlockSpec(memory_space=pltpu.VMEM)] * 7,
        scratch_shapes=[
            pltpu.VMEM((FEATS, 3 * LANES), BF16),
            pltpu.VMEM((3 * LANES, FEATS), F32),
            pltpu.VMEM((2, 4, PADDED, FEATS), BF16),
            pltpu.VMEM((2, 2, PADDED, FEATS), BF16),
            pltpu.VMEM((RING, RING, *block), BF16),
            pltpu.VMEM(block, BF16),
            pltpu.VMEM((RING, 2, 4, *units), BF16),
            pltpu.VMEM((6, 4, *units), BF16),
            pltpu.VMEM((4, *units), BF16),
            pltpu.VMEM((4, *units), BF16),
            pltpu.VMEM((4, *units), F32),
            pltpu.VMEM((RING, 2, 2, *units), BF16),
            pltpu.VMEM((RING, RING, 2, *block), BF16),
            pltpu.VMEM((6, RING, *block), BF16),
            pltpu.VMEM((RING, 2, *block), BF16),
            pltpu.VMEM((6, *block), BF16),
            pltpu.VMEM((2, *block), F32),
            pltpu.VMEM((RING, RING, 2, *block), BF16),
            pltpu.VMEM((RING, 2, 2, *units), BF16),
            pltpu.VMEM((6, 2, *units), BF16),
            pltpu.VMEM((2, *units), BF16),
            pltpu.VMEM((2, *units), BF16),
            pltpu.VMEM((2, *units), F32),
            pltpu.VMEM((RING, 2, 4, *units), BF16),
            pltpu.VMEM((2, 4, PADDED, FEATS), F32),
            pltpu.VMEM((4, PADDED, FEATS), F32),
            pltpu.VMEM((2, 2, PADDED, FEATS), F32),
            pltpu.VMEM((2, PADDED, FEATS), F32),
            pltpu.VMEM((6, 8, LANES), F32),
            pltpu.VMEM((5, 3, 8, LANES), F32),
            pltpu.SemaphoreType.DMA((SLOTS,)),
            pltpu.SemaphoreType.DMA((SLOTS,)),
        ],
        compiler_params=pltpu.CompilerParams(
            collective_id=0, has_side_effects=True, vmem_limit_bytes=60 * 1024 * 1024
        ),
    )(*operands)


def body(
    tokens,
    target,
    gate_weight,
    up_weight,
    down_weight,
    probe_gate,
    probe_up,
    probe_down,
    first_gate,
    first_up,
    first_down,
    second_gate,
    second_up,
    second_down,
):
    grad_gate, grad_up, grad_down, curv_gate, curv_up, curv_down, sums = whole_step(
        tokens, target, gate_weight, up_weight, down_weight, probe_gate, probe_up, probe_down
    )
    count = 3.0 * D * FF
    rms_grad = jnp.sqrt(sums[0, 0] / count + 1e-06)
    rms_curv = jnp.sqrt(sums[0, 1] / count + 1e-06)
    fix_first = 1.0 - 0.9**STEP
    fix_second = 1.0 - 0.95**STEP
    firsts = []
    seconds = []
    updates = []
    for grad, curv, first, second in (
        (grad_gate, curv_gate, first_gate, second_gate),
        (grad_up, curv_up, first_up, second_up),
        (grad_down, curv_down, first_down, second_down),
    ):
        new_first = 0.9 * first + 0.1 * (grad / rms_grad)
        scaled = curv / rms_curv
        new_second = 0.95 * second + 0.05 * (scaled * scaled)
        firsts.append(new_first)
        seconds.append(new_second)
        updates.append(new_first / fix_first / (jnp.sqrt(new_second / fix_second) + 1e-08))
    return (*firsts, *seconds, *updates)


def solution(mesh):
    torus = Mesh(mesh.devices.reshape(4, 2, 2, 4, 4), (*ROW, *COL))
    feats, units = P(ROW, COL), P(COL, ROW)
    in_specs = (units, units, feats, feats, units) + (feats, feats, units) * 3
    out_specs = (feats, feats, units) * 3
    return jax.shard_map(body, mesh=torus, in_specs=in_specs, out_specs=out_specs, check_vma=False)
```

```python
import jax
import jax.numpy as jnp
from jax import lax
from jax.experimental import pallas as pl
from jax.experimental.pallas import tpu as pltpu
from jax.sharding import Mesh
from jax.sharding import PartitionSpec as P

D = 4096
FF = 5504
STEP = 10
COL = ("col_0", "col_1")
ROW = ("row_0", "row_1", "row_2")
RING = 4
UNITS = 344
PADDED = 352
FEATS = 256
HALF = 64
LANES = 128
STRIP = 32
MESH = pl.DeviceIdType.MESH
BF16 = jnp.bfloat16
F32 = jnp.float32

X_AXIS, Z_AXIS, CORE_AXIS = ROW
H_AXIS, Y_AXIS = COL


def dot_nn(left, right):
    return jnp.dot(left, right, preferred_element_type=F32)


def dot_nt(left, right):
    return lax.dot_general(left, right, (((1,), (1,)), ((), ())), preferred_element_type=F32)


def dot_tn(left, right):
    return lax.dot_general(left, right, (((0,), (0,)), ((), ())), preferred_element_type=F32)


def block_ones(size):
    rows = lax.broadcasted_iota(jnp.int32, (size, size), 0) >> 2
    cols = lax.broadcasted_iota(jnp.int32, (size, size), 1) >> 2
    return jnp.where(rows == cols, 1.0, 0.0).astype(BF16)


def two_terms(values):
    high = values.astype(BF16)
    low = (values - high.astype(F32)).astype(BF16)
    return high, low


def curvature(sign, hess):
    high, low = two_terms(jnp.abs(sign * hess))
    ones = block_ones(hess.shape[0])
    down = dot_nn(ones, high) + dot_nn(ones, low)
    high, low = two_terms(down)
    ones = block_ones(hess.shape[1])
    return (dot_nn(high, ones) + dot_nn(low, ones)) * 0.0625


class Copies:
    def __init__(self, send_sems, recv_sems):
        self.send_sems = send_sems
        self.recv_sems = recv_sems
        self.next = 0
        self.pending = []

    def slots(self, count):
        first = self.next
        self.next += count
        return first

    def copy(self, src, dst, slot, peer):
        return pltpu.make_async_remote_copy(
            src_ref=src,
            dst_ref=dst,
            send_sem=self.send_sems.at[slot],
            recv_sem=self.recv_sems.at[slot],
            device_id=peer,
            device_id_type=MESH,
        )

    def send(self, src, dst, slot, peer):
        self.copy(src, dst, slot, peer).start()

    def arrived(self, dst, slot, peer):
        self.copy(dst, dst, slot, peer).wait_recv()

    def sent(self, src, slot, peer):
        self.copy(src, src, slot, peer).wait_send()


def around(axis):
    here = lax.axis_index(axis)
    return here, lax.rem(here + 1, RING), lax.rem(here + 3, RING), lax.rem(here + 2, RING)


def add_strips(dst, terms):
    def strip(index, carry):
        rows = pl.ds(pl.multiple_of(index * STRIP, STRIP), STRIP)
        total = terms[0][rows, :].astype(F32)
        for term in terms[1:]:
            total = total + term[rows, :].astype(F32)
        dst[rows, :] = total.astype(dst.dtype)
        return carry

    lax.fori_loop(0, PADDED // STRIP, strip, 0)


def add_blocks(dst, terms):
    for part in range(2):
        total = terms[0][part].astype(F32)
        for term in terms[1:]:
            total = total + term[part].astype(F32)
        dst[part] = total.astype(dst.dtype)


class RingSum:
    def __init__(self, copies, axis, count, block, landed, add):
        self.copies, self.axis, self.block, self.landed, self.add = copies, axis, block, landed, add
        self.base = copies.slots(6 * count)
        self.count = count
        self.here, self.plus, self.minus, self.opposite = around(axis)

    def slot(self, kind, index):
        return self.base + kind * self.count + index

    def send(self, src, kind, index, peer):
        self.copies.send(src, self.landed(kind, index), self.slot(kind, index), {self.axis: peer})

    def wait(self, kind, index):
        ref = self.landed(kind, index)
        self.copies.arrived(ref, self.slot(kind, index), {self.axis: self.plus})

    def send_for(self, place, index):
        role = lax.rem(place - self.here + RING, RING)

        @pl.when(role == 1)
        def _():
            self.send(self.block(place, 1, index), 3, index, self.plus)

        @pl.when(role == 2)
        def _():
            self.send(self.block(place, 0, index), 0, index, self.plus)
            self.send(self.block(place, 1, index), 1, index, self.minus)

        @pl.when(role == 3)
        def _():
            self.send(self.block(place, 0, index), 4, index, self.minus)

    def send_opposite(self, index):
        self.send(self.block(self.opposite, 0, index), 0, index, self.plus)
        self.send(self.block(self.opposite, 1, index), 1, index, self.minus)

    def send_plus(self, index):
        self.send(self.block(self.plus, 1, index), 3, index, self.plus)

    def send_minus(self, index):
        self.send(self.block(self.minus, 0, index), 4, index, self.minus)

    def forward(self, index):
        self.wait(0, index)
        ref = self.block(self.plus, 0, index)
        self.add(ref, (ref, self.landed(0, index)))
        self.send(ref, 2, index, self.plus)
        self.wait(1, index)
        ref = self.block(self.minus, 1, index)
        self.add(ref, (ref, self.landed(1, index)))
        self.send(ref, 5, index, self.minus)

    def wait_terms(self, index):
        for kind in (3, 4, 2, 5):
            self.wait(kind, index)

    def terms(self, half, index):
        return (
            self.block(self.here, half, index),
            self.landed(2 + half, index),
            self.landed(4 + half, index),
        )

    def drain(self, index):
        for kind in range(6):
            self.copies.sent(
                self.landed(kind, index), self.slot(kind, index), {self.axis: self.plus}
            )


class RowSum:
    def __init__(self, copies, count, blocks, landed, pair_sums, pair_landed):
        self.copies, self.count = copies, count
        self.ring = RingSum(
            copies,
            X_AXIS,
            count,
            lambda place, half, index: blocks.at[place, half, index],
            lambda kind, index: landed.at[kind, index],
            add_strips,
        )
        self.base = copies.slots(count)
        self.pair_sums, self.pair_landed = pair_sums, pair_landed
        self.z = lax.axis_index(Z_AXIS)
        self.other = 1 - self.z

    def pair(self, index):
        self.ring.wait_terms(index)
        add_strips(self.pair_sums.at[index], self.ring.terms(self.other, index))
        self.copies.send(
            self.pair_sums.at[index],
            self.pair_landed.at[index],
            self.base + index,
            {Z_AXIS: self.other},
        )

    def finish(self, dst, index):
        self.copies.arrived(self.pair_landed.at[index], self.base + index, {Z_AXIS: self.other})
        add_strips(dst, (*self.ring.terms(self.z, index), self.pair_landed.at[index]))

    def drain(self, index):
        self.ring.drain(index)
        self.copies.sent(self.pair_sums.at[index], self.base + index, {Z_AXIS: self.other})


class RowGather:
    def __init__(self, copies, count, buffer):
        self.copies, self.count, self.buffer = copies, count, buffer
        self.base = copies.slots(7 * count)
        self.here, self.plus, self.minus, self.opposite = around(X_AXIS)
        self.z = lax.axis_index(Z_AXIS)
        self.other = 1 - self.z

    def send(self, place, z, kind, index, peer):
        ref = self.buffer.at[place, z, index]
        self.copies.send(ref, ref, self.base + kind * self.count + index, peer)

    def wait(self, place, z, kind, index):
        ref = self.buffer.at[place, z, index]
        slot = self.base + kind * self.count + index
        self.copies.arrived(ref, slot, {Z_AXIS: self.other})

    def start(self, index):
        self.send(self.here, self.z, 0, index, {Z_AXIS: self.other})
        self.send(self.here, self.z, 1, index, {X_AXIS: self.plus})
        self.send(self.here, self.z, 2, index, {X_AXIS: self.minus})

    def pair(self, index):
        self.wait(self.here, self.other, 0, index)
        self.send(self.here, self.other, 3, index, {X_AXIS: self.plus})
        self.send(self.here, self.other, 4, index, {X_AXIS: self.minus})

    def forward(self, index):
        self.wait(self.minus, self.z, 1, index)
        self.wait(self.minus, self.other, 3, index)
        self.send(self.minus, 0, 5, index, {X_AXIS: self.plus})
        self.wait(self.plus, self.z, 2, index)
        self.wait(self.plus, self.other, 4, index)
        self.send(self.plus, 1, 6, index, {X_AXIS: self.minus})

    def finish(self, index):
        self.wait(self.opposite, 0, 5, index)
        self.wait(self.opposite, 1, 6, index)

    def drain(self, index):
        for kind in range(7):
            ref = self.buffer.at[0, 0, index]
            slot = self.base + kind * self.count + index
            self.copies.sent(ref, slot, {Z_AXIS: self.other})


class RingGather:
    def __init__(self, copies, axis, whole, half):
        self.copies, self.axis, self.whole, self.half = copies, axis, whole, half
        self.base = copies.slots(4)
        self.here, self.plus, self.minus, self.opposite = around(axis)

    def send(self, ref, kind, peer):
        self.copies.send(ref, ref, self.base + kind, {self.axis: peer})

    def wait(self, ref, kind):
        self.copies.arrived(ref, self.base + kind, {self.axis: self.plus})

    def start(self):
        self.send(self.whole(self.here), 0, self.plus)
        self.send(self.whole(self.here), 1, self.minus)

    def from_minus(self):
        self.wait(self.whole(self.minus), 0)
        self.send(self.half(self.minus, 0), 2, self.plus)

    def from_plus(self):
        self.wait(self.whole(self.plus), 1)
        self.send(self.half(self.plus, 1), 3, self.minus)

    def forward(self):
        self.from_minus()
        self.from_plus()

    def finish(self):
        self.wait(self.half(self.opposite, 0), 2)
        self.wait(self.half(self.opposite, 1), 3)

    def drain(self):
        for kind in range(4):
            ref = self.whole(0) if kind < 2 else self.half(0, 0)
            self.copies.sent(ref, self.base + kind, {self.axis: self.plus})


class ColGather:
    def __init__(self, copies, buffer):
        here, plus, minus, opposite = around(H_AXIS)
        y = lax.axis_index(Y_AXIS)
        self.outer = RingGather(
            copies,
            H_AXIS,
            lambda place: buffer.at[place, y],
            lambda place, half: buffer.at[place, y, half],
        )
        self.inner = [
            RingGather(
                copies,
                Y_AXIS,
                lambda place, layer=layer: buffer.at[layer, place],
                lambda place, half, layer=layer: buffer.at[layer, place, half],
            )
            for layer in (here, minus, plus, opposite)
        ]
        self.places = (here, minus, plus, opposite)

    def start(self):
        self.outer.start()
        self.inner[0].start()

    def run(self, use):
        here, minus, plus, opposite = self.inner
        here.forward()
        self.outer.from_minus()
        minus.start()
        self.outer.from_plus()
        plus.start()
        here.finish()
        use(self.places[0])
        minus.forward()
        plus.forward()
        self.outer.finish()
        opposite.start()
        minus.finish()
        use(self.places[1])
        plus.finish()
        use(self.places[2])
        opposite.forward()
        opposite.finish()
        use(self.places[3])

    def drain(self):
        self.outer.drain()
        for inner in self.inner:
            inner.drain()


def step_kernel(
    tokens,
    target,
    gate_weight,
    up_weight,
    down_weight,
    probe_gate,
    probe_up,
    probe_down,
    grad_gate_out,
    grad_up_out,
    grad_down_out,
    curv_gate_out,
    curv_up_out,
    curv_down_out,
    sums_out,
    proj,
    down,
    x,
    tgt,
    part,
    part_landed,
    pair_sums,
    pair_landed,
    pre,
    hid,
    outs,
    outs_landed,
    layer_sums,
    layer_landed,
    final,
    err,
    back,
    back_landed,
    back_pair,
    back_pair_landed,
    d_hid,
    d_pre,
    grads,
    grads_landed,
    grads_down,
    grads_down_landed,
    tiles,
    tiles_landed,
    send_sems,
    recv_sems,
):
    copies = Copies(send_sems, recv_sems)
    core = lax.axis_index(CORE_AXIS)
    other_core = 1 - core
    x_here, x_plus, x_minus, x_opposite = around(X_AXIS)
    y_here, y_plus, y_minus, y_opposite = around(Y_AXIS)
    h_here, h_plus, h_minus, h_opposite = around(H_AXIS)
    z_here = lax.axis_index(Z_AXIS)
    partner = {CORE_AXIS: other_core}

    barrier = pltpu.get_barrier_semaphore()
    peers = [partner, {Z_AXIS: 1 - z_here}]
    for axis in (X_AXIS, Y_AXIS, H_AXIS):
        peers += [{axis: place} for place in around(axis)[1:]]
    for peer in peers:
        pl.semaphore_signal(barrier, inc=1, device_id=peer, device_id_type=MESH)

    own_rows = pl.ds(pl.multiple_of(core * HALF, HALF), HALF)
    other_rows = pl.ds(pl.multiple_of(other_core * HALF, HALF), HALF)
    x[h_here, y_here, core] = tokens[own_rows, :]
    tgt[core] = target[own_rows, :]

    def sign(ref):
        return (2 * ref[...] - 1).astype(F32).astype(BF16)

    def lay_out(dst, index, values):
        dst[core, index, PADDED - 32 :] = jnp.zeros((32, FEATS), BF16)
        dst[core, index, :UNITS] = values

    lay_out(proj, 0, gate_weight[...])
    lay_out(proj, 1, up_weight[...])
    lay_out(proj, 2, sign(probe_gate))
    lay_out(proj, 3, sign(probe_up))
    lay_out(down, 0, down_weight[...])
    lay_out(down, 1, sign(probe_down))

    pl.semaphore_wait(barrier, len(peers))
    near = copies.slots(9)
    copies.send(tokens.at[other_rows], x.at[h_here, y_here, core], near, partner)
    copies.send(proj.at[core], proj.at[core], near + 1, partner)
    copies.send(target.at[other_rows], tgt.at[core], near + 2, partner)
    copies.send(down.at[core], down.at[core], near + 3, partner)

    copies.arrived(x.at[h_here, y_here, other_core], near, partner)
    x_gather = ColGather(copies, x)
    x_gather.start()
    copies.arrived(proj.at[other_core], near + 1, partner)

    def token_block(ref, place, *rest):
        return [
            ref[(place, slice(None), *rest, half)].reshape(RING * HALF, FEATS) for half in range(2)
        ]

    row_sum = RowSum(copies, 4, part, part_landed, pair_sums, pair_landed)

    def project(index, place):
        left, right = token_block(x, place)
        both = dot_nt(proj[0, index], left) + dot_nt(proj[1, index], right)
        both = both.astype(BF16)
        part[place, 0, index] = both[:, :LANES]
        part[place, 1, index] = both[:, LANES:]

    def each(count, step):
        def body(index, carry):
            step(index)
            return carry

        lax.fori_loop(0, count, body, 0)

    def project_and_send(place):
        def one(index):
            project(index, place)
            row_sum.ring.send_for(place, index)

        each(4, one)

    x_gather.run(project_and_send)
    each(4, row_sum.ring.forward)
    each(4, row_sum.pair)

    def strips(step):
        def body(index, carry):
            step(pl.ds(pl.multiple_of(index * STRIP, STRIP), STRIP))
            return carry

        lax.fori_loop(0, PADDED // STRIP, body, 0)

    def hide(rows):
        pre_gate, pre_up = pre[0, rows, :], pre[1, rows, :]
        act = pre_gate * jax.nn.sigmoid(pre_gate)
        hid[x_here, z_here, 0, rows, :] = (act * pre_up).astype(BF16)

    def hide_dot(rows):
        pre_gate, pre_up = pre[0, rows, :], pre[1, rows, :]
        dot_gate, dot_up = pre[2, rows, :], pre[3, rows, :]
        sig = jax.nn.sigmoid(pre_gate)
        act = pre_gate * sig
        slope = sig * (1.0 + pre_gate * (1.0 - sig))
        hid[x_here, z_here, 1, rows, :] = (slope * dot_gate * pre_up + act * dot_up).astype(BF16)

    hid_gather = RowGather(copies, 2, hid)
    each(2, lambda index: row_sum.finish(pre.at[index], index))
    strips(hide)
    hid_gather.start(0)
    each(2, lambda index: row_sum.finish(pre.at[2 + index], 2 + index))
    strips(hide_dot)
    hid_gather.start(1)
    each(2, hid_gather.pair)
    copies.arrived(down.at[other_core], near + 3, partner)

    out_sum = RingSum(
        copies,
        Y_AXIS,
        4,
        lambda place, half, layer: outs.at[layer[1], place, half],
        lambda kind, layer: outs_landed.at[kind, layer[0]],
        add_blocks,
    )
    out_sum.slot = lambda kind, layer: out_sum.base + kind * 4 + layer[0]

    def whole_units(ref, place, index):
        return jnp.concatenate([ref[place, 0, index], ref[place, 1, index]], axis=1)

    def expand(place):
        plain = whole_units(hid, place, 0)
        tangent = whole_units(hid, place, 1)
        for half in range(2):
            value = dot_tn(plain, down[half, 0])
            along = dot_tn(tangent, down[half, 0]) + dot_tn(plain, down[half, 1])
            value = value.astype(BF16).reshape(RING, HALF, FEATS)
            along = along.astype(BF16).reshape(RING, HALF, FEATS)
            for block in range(RING):
                outs[place, block, 0, half] = value[block]
                outs[place, block, 1, half] = along[block]

    layers = [(0, x_here), (1, x_minus), (2, x_plus), (3, x_opposite)]

    def expand_and_send(layer):
        expand(layer[1])
        out_sum.send_opposite(layer)
        out_sum.send_plus(layer)
        out_sum.send_minus(layer)

    layer_sum = RingSum(
        copies,
        H_AXIS,
        1,
        lambda place, half, index: layer_sums.at[place, half],
        lambda kind, index: layer_landed.at[kind],
        add_blocks,
    )

    def complete(layer):
        out_sum.wait_terms(layer)
        for half in range(2):
            add_blocks(layer_sums.at[layer[1], half], out_sum.terms(half, layer))
        layer_sum.send_for(layer[1], 0)

    expand_and_send(layers[0])
    each(2, hid_gather.forward)
    out_sum.forward(layers[0])
    expand_and_send(layers[1])
    expand_and_send(layers[2])
    complete(layers[0])
    out_sum.forward(layers[1])
    out_sum.forward(layers[2])
    each(2, hid_gather.finish)
    expand_and_send(layers[3])
    complete(layers[1])
    complete(layers[2])
    out_sum.forward(layers[3])
    complete(layers[3])
    layer_sum.forward(0)
    layer_sum.wait_terms(0)
    copies.arrived(tgt.at[other_core], near + 2, partner)
    for half in range(2):
        add_blocks(final.at[half], layer_sum.terms(half, 0))
    for side in range(2):
        value = final[0, side] - tgt[side].astype(F32)
        err[h_here, y_here, 0, side] = value.astype(BF16)
        err[h_here, y_here, 1, side] = final[1, side].astype(BF16)

    err_gather = ColGather(copies, err)
    err_gather.start()

    back_sum = RowSum(copies, 2, back, back_landed, back_pair, back_pair_landed)

    def turn_back(place):
        plain = token_block(err, place, 0)
        tangent = token_block(err, place, 1)
        value = dot_nt(down[0, 0], plain[0]) + dot_nt(down[1, 0], plain[1])
        along = dot_nt(down[0, 0], tangent[0]) + dot_nt(down[1, 0], tangent[1])
        along = along + dot_nt(down[0, 1], plain[0]) + dot_nt(down[1, 1], plain[1])
        for index, whole in enumerate((value, along)):
            whole = whole.astype(BF16)
            back[place, 0, index] = whole[:, :LANES]
            back[place, 1, index] = whole[:, LANES:]

    def turn_back_and_send(place):
        turn_back(place)
        each(2, lambda index: back_sum.ring.send_for(place, index))

    err_gather.run(turn_back_and_send)
    each(2, back_sum.ring.forward)
    each(2, back_sum.pair)
    each(2, lambda index: back_sum.finish(d_hid.at[index], index))

    def slopes(rows):
        pre_gate, pre_up = pre[0, rows, :], pre[1, rows, :]
        dot_gate, dot_up = pre[2, rows, :], pre[3, rows, :]
        d_hidden, d_hidden_dot = d_hid[0, rows, :], d_hid[1, rows, :]
        sig = jax.nn.sigmoid(pre_gate)
        act = pre_gate * sig
        slope = sig * (1.0 + pre_gate * (1.0 - sig))
        bend = sig * (1.0 - sig) * (2.0 + pre_gate * (1.0 - 2.0 * sig))
        dd_gate = (
            d_hidden_dot * pre_up * slope
            + d_hidden * dot_up * slope
            + d_hidden * pre_up * bend * dot_gate
        )
        dd_up = d_hidden_dot * act + d_hidden * slope * dot_gate
        d_pre[x_here, z_here, 0, rows, :] = (d_hidden * pre_up * slope).astype(BF16)
        d_pre[x_here, z_here, 1, rows, :] = (d_hidden * act).astype(BF16)
        d_pre[x_here, z_here, 2, rows, :] = dd_gate.astype(BF16)
        d_pre[x_here, z_here, 3, rows, :] = dd_up.astype(BF16)

    strips(slopes)
    pre_gather = RowGather(copies, 4, d_pre)
    each(4, pre_gather.start)
    each(4, pre_gather.pair)
    each(4, pre_gather.forward)

    def down_grads(side):
        plain_sum = jnp.zeros((PADDED, FEATS), F32)
        along_sum = jnp.zeros((PADDED, FEATS), F32)
        for place in range(RING):
            plain = whole_units(hid, place, 0)
            tangent = whole_units(hid, place, 1)
            err_block = err[place, :, 0, side].reshape(RING * HALF, FEATS)
            dot_block = err[place, :, 1, side].reshape(RING * HALF, FEATS)
            plain_sum = plain_sum + dot_nn(plain, err_block)
            along_sum = along_sum + dot_nn(tangent, err_block) + dot_nn(plain, dot_block)
        grads_down[side, 0] = plain_sum
        grads_down[side, 1] = along_sum

    down_grads(other_core)
    copies.send(grads_down.at[other_core], grads_down_landed, near + 4, partner)
    down_grads(core)

    def tokens_of(place, side):
        return x[place, :, side].reshape(RING * HALF, FEATS)

    def first_grads(side):
        def one(index):
            total = dot_nn(whole_units(d_pre, x_here, index), tokens_of(x_here, side))
            for place in (x_minus, x_plus):
                total = total + dot_nn(whole_units(d_pre, place, index), tokens_of(place, side))
            grads[side, index] = total

        each(4, one)

    def last_grads(side, index):
        last = dot_nn(whole_units(d_pre, x_opposite, index), tokens_of(x_opposite, side))
        grads[side, index] = grads[side, index] + last

    first_grads(other_core)
    first_grads(core)

    def squares(values):
        return jnp.sum(values * values, axis=0, keepdims=True)

    copies.arrived(grads_down_landed, near + 4, partner)
    grad = grads_down[core, 0] + grads_down_landed[0]
    hess = grads_down[core, 1] + grads_down_landed[1]
    grad_down_out[...] = grad[:UNITS]
    grad_sum = squares(grad)
    curv = curvature(down[core, 1].astype(F32), hess)
    curv_down_out[...] = curv[:UNITS]
    curv_sum = squares(curv)

    def last_and_send(index):
        pre_gather.finish(index)
        last_grads(other_core, index)
        copies.send(grads.at[other_core, index], grads_landed.at[index], near + 5 + index, partner)

    each(4, last_and_send)
    each(4, lambda index: last_grads(core, index))

    for index, (grad_out, curv_out) in enumerate(
        ((grad_gate_out, curv_gate_out), (grad_up_out, curv_up_out))
    ):
        copies.arrived(grads_landed.at[index], near + 5 + index, partner)
        grad = grads[core, index] + grads_landed[index]
        grad_out[...] = grad[:UNITS]
        grad_sum = grad_sum + squares(grad)
        copies.arrived(grads_landed.at[2 + index], near + 7 + index, partner)
        hess = grads[core, 2 + index] + grads_landed[2 + index]
        curv = curvature(proj[core, 2 + index].astype(F32), hess)
        curv_out[...] = curv[:UNITS]
        curv_sum = curv_sum + squares(curv)

    lane = lax.broadcasted_iota(jnp.int32, (8, LANES), 1)
    grad_sum = jnp.sum(grad_sum, axis=1, keepdims=True)
    curv_sum = jnp.sum(curv_sum, axis=1, keepdims=True)
    tiles[0] = jnp.where(lane == 0, grad_sum, jnp.where(lane == 1, curv_sum, 0.0))

    stages = [
        [partner],
        [{Z_AXIS: 1 - z_here}],
        [{X_AXIS: x_plus}, {X_AXIS: x_opposite}, {X_AXIS: x_minus}],
        [{Y_AXIS: y_plus}, {Y_AXIS: y_opposite}, {Y_AXIS: y_minus}],
        [{H_AXIS: h_plus}, {H_AXIS: h_opposite}, {H_AXIS: h_minus}],
    ]
    small = copies.slots(3 * len(stages))
    for stage, receivers in enumerate(stages):
        for index, peer in enumerate(receivers):
            slot = small + 3 * stage + index
            copies.send(tiles.at[stage], tiles_landed.at[stage, index], slot, peer)
        total = tiles[stage]
        for index, peer in enumerate(receivers):
            copies.arrived(tiles_landed.at[stage, index], small + 3 * stage + index, peer)
            total = total + tiles_landed[stage, index]
        tiles[stage + 1] = total
    sums_out[...] = tiles[len(stages)]

    copies.sent(x.at[0, 0, 0], near, partner)
    copies.sent(proj.at[0], near + 1, partner)
    copies.sent(tgt.at[0], near + 2, partner)
    copies.sent(down.at[0], near + 3, partner)
    copies.sent(grads_down_landed, near + 4, partner)
    each(4, lambda index: copies.sent(grads_landed.at[index], near + 5 + index, partner))
    x_gather.drain()
    err_gather.drain()
    each(4, row_sum.drain)
    each(2, back_sum.drain)
    each(2, hid_gather.drain)
    each(4, pre_gather.drain)
    for layer in layers:
        out_sum.drain(layer)
    layer_sum.drain(0)
    for stage, receivers in enumerate(stages):
        for index, peer in enumerate(receivers):
            copies.sent(tiles.at[stage], small + 3 * stage + index, peer)


SLOTS = 240


def whole_step(*operands):
    units = (PADDED, LANES)
    block = (2, HALF, FEATS)
    return pl.pallas_call(
        step_kernel,
        out_shape=(
            *[jax.ShapeDtypeStruct((UNITS, FEATS), F32)] * 6,
            jax.ShapeDtypeStruct((8, LANES), F32),
        ),
        in_specs=[pl.BlockSpec(memory_space=pltpu.VMEM)] * 8,
        out_specs=[pl.BlockSpec(memory_space=pltpu.VMEM)] * 7,
        scratch_shapes=[
            pltpu.VMEM((2, 4, PADDED, FEATS), BF16),
            pltpu.VMEM((2, 2, PADDED, FEATS), BF16),
            pltpu.VMEM((RING, RING, *block), BF16),
            pltpu.VMEM(block, BF16),
            pltpu.VMEM((RING, 2, 4, *units), BF16),
            pltpu.VMEM((6, 4, *units), BF16),
            pltpu.VMEM((4, *units), BF16),
            pltpu.VMEM((4, *units), BF16),
            pltpu.VMEM((4, *units), F32),
            pltpu.VMEM((RING, 2, 2, *units), BF16),
            pltpu.VMEM((RING, RING, 2, *block), BF16),
            pltpu.VMEM((6, RING, *block), BF16),
            pltpu.VMEM((RING, 2, *block), BF16),
            pltpu.VMEM((6, *block), BF16),
            pltpu.VMEM((2, *block), F32),
            pltpu.VMEM((RING, RING, 2, *block), BF16),
            pltpu.VMEM((RING, 2, 2, *units), BF16),
            pltpu.VMEM((6, 2, *units), BF16),
            pltpu.VMEM((2, *units), BF16),
            pltpu.VMEM((2, *units), BF16),
            pltpu.VMEM((2, *units), F32),
            pltpu.VMEM((RING, 2, 4, *units), BF16),
            pltpu.VMEM((2, 4, PADDED, FEATS), F32),
            pltpu.VMEM((4, PADDED, FEATS), F32),
            pltpu.VMEM((2, 2, PADDED, FEATS), F32),
            pltpu.VMEM((2, PADDED, FEATS), F32),
            pltpu.VMEM((6, 8, LANES), F32),
            pltpu.VMEM((5, 3, 8, LANES), F32),
            pltpu.SemaphoreType.DMA((SLOTS,)),
            pltpu.SemaphoreType.DMA((SLOTS,)),
        ],
        compiler_params=pltpu.CompilerParams(
            collective_id=0, has_side_effects=True, vmem_limit_bytes=60 * 1024 * 1024
        ),
    )(*operands)


def body(
    tokens,
    target,
    gate_weight,
    up_weight,
    down_weight,
    probe_gate,
    probe_up,
    probe_down,
    first_gate,
    first_up,
    first_down,
    second_gate,
    second_up,
    second_down,
):
    grad_gate, grad_up, grad_down, curv_gate, curv_up, curv_down, sums = whole_step(
        tokens, target, gate_weight.T, up_weight.T, down_weight, probe_gate.T, probe_up.T, probe_down
    )
    count = 3.0 * D * FF
    rms_grad = jnp.sqrt(sums[0, 0] / count + 1e-06)
    rms_curv = jnp.sqrt(sums[0, 1] / count + 1e-06)
    fix_first = 1.0 - 0.9**STEP
    fix_second = 1.0 - 0.95**STEP
    firsts = []
    seconds = []
    updates = []
    for grad, curv, first, second in (
        (grad_gate, curv_gate, first_gate.T, second_gate.T),
        (grad_up, curv_up, first_up.T, second_up.T),
        (grad_down, curv_down, first_down, second_down),
    ):
        new_first = 0.9 * first + 0.1 * (grad / rms_grad)
        scaled = curv / rms_curv
        new_second = 0.95 * second + 0.05 * (scaled * scaled)
        firsts.append(new_first)
        seconds.append(new_second)
        updates.append(new_first / fix_first / (jnp.sqrt(new_second / fix_second) + 1e-08))
    outs = (firsts, seconds, updates)
    return tuple(value for gate, up, down in outs for value in (gate.T, up.T, down))


def solution(mesh):
    torus = Mesh(mesh.devices.reshape(4, 2, 2, 4, 4), (*ROW, *COL))
    feats, units = P(ROW, COL), P(COL, ROW)
    in_specs = (units, units, feats, feats, units) + (feats, feats, units) * 3
    out_specs = (feats, feats, units) * 3
    return jax.shard_map(body, mesh=torus, in_specs=in_specs, out_specs=out_specs, check_vma=False)
```

```python
import jax
import jax.numpy as jnp
from jax import lax
from jax.experimental import pallas as pl
from jax.experimental.pallas import tpu as pltpu
from jax.sharding import Mesh
from jax.sharding import PartitionSpec as P

D = 4096
FF = 5504
STEP = 10
COL = ("col_0", "col_1")
ROW = ("row_0", "row_1", "row_2")
RING = 4
UNITS = 344
PADDED = 352
FEATS = 256
HALF = 64
LANES = 128
STRIP = 32
MESH = pl.DeviceIdType.MESH
BF16 = jnp.bfloat16
F32 = jnp.float32

X_AXIS, Z_AXIS, CORE_AXIS = ROW
H_AXIS, Y_AXIS = COL


def dot_nn(left, right):
    return jnp.dot(left, right, preferred_element_type=F32)


def dot_nt(left, right):
    return lax.dot_general(left, right, (((1,), (1,)), ((), ())), preferred_element_type=F32)


def dot_tn(left, right):
    return lax.dot_general(left, right, (((0,), (0,)), ((), ())), preferred_element_type=F32)


def block_ones(size):
    rows = lax.broadcasted_iota(jnp.int32, (size, size), 0) >> 2
    cols = lax.broadcasted_iota(jnp.int32, (size, size), 1) >> 2
    return jnp.where(rows == cols, 1.0, 0.0).astype(BF16)


def two_terms(values):
    high = values.astype(BF16)
    low = (values - high.astype(F32)).astype(BF16)
    return high, low


def curvature(sign, hess):
    high, low = two_terms(jnp.abs(sign * hess))
    ones = block_ones(hess.shape[0])
    down = dot_nn(ones, high) + dot_nn(ones, low)
    high, low = two_terms(down)
    ones = block_ones(hess.shape[1])
    return (dot_nn(high, ones) + dot_nn(low, ones)) * 0.0625


class Copies:
    def __init__(self, send_sems, recv_sems):
        self.send_sems = send_sems
        self.recv_sems = recv_sems
        self.next_in = 0
        self.next_out = 0

    def slots(self, count):
        self.next_in += count
        return self.next_in - count

    def outs(self, count):
        self.next_out += count
        return self.next_out - count

    def copy(self, src, dst, out, slot, peer):
        return pltpu.make_async_remote_copy(
            src_ref=src,
            dst_ref=dst,
            send_sem=self.send_sems.at[out],
            recv_sem=self.recv_sems.at[slot],
            device_id=peer,
            device_id_type=MESH,
        )

    def send(self, src, dst, out, slot, peer):
        self.copy(src, dst, out, slot, peer).start()

    def arrived(self, dst, slot, peer):
        self.copy(dst, dst, 0, slot, peer).wait_recv()

    def sent(self, src, out, peer):
        self.copy(src, src, out, 0, peer).wait_send()


def around(axis):
    here = lax.axis_index(axis)
    return here, lax.rem(here + 1, RING), lax.rem(here + 3, RING), lax.rem(here + 2, RING)


def add_strips(dst, terms):
    def strip(index, carry):
        rows = pl.ds(pl.multiple_of(index * STRIP, STRIP), STRIP)
        total = terms[0][rows, :].astype(F32)
        for term in terms[1:]:
            total = total + term[rows, :].astype(F32)
        dst[rows, :] = total.astype(dst.dtype)
        return carry

    lax.fori_loop(0, PADDED // STRIP, strip, 0)


def add_blocks(dst, terms):
    total = terms[0][...].astype(F32)
    for term in terms[1:]:
        total = total + term[...].astype(F32)
    dst[...] = total.astype(dst.dtype)


class RingSum:
    def __init__(self, copies, axis, count, block, landed, all_landed, number=lambda index: index):
        self.number, self.all_landed = number, all_landed
        self.out = copies.outs(6)
        self.copies, self.axis, self.block, self.landed = copies, axis, block, landed
        self.base = copies.slots(6 * count)
        self.count = count
        self.here, self.plus, self.minus, self.opposite = around(axis)

    def slot(self, kind, index):
        return self.base + kind * self.count + self.number(index)

    def send(self, src, kind, index, peer):
        slot = self.slot(kind, index)
        self.copies.send(src, self.landed(kind, index), self.out + kind, slot, {self.axis: peer})

    def wait(self, kind, index):
        ref = self.landed(kind, index)
        self.copies.arrived(ref, self.slot(kind, index), {self.axis: self.plus})

    def send_for(self, place, index):
        role = lax.rem(place - self.here + RING, RING)

        @pl.when(role == 1)
        def _():
            self.send(self.block(place, 1, index), 3, index, self.plus)

        @pl.when(role == 2)
        def _():
            self.send(self.block(place, 0, index), 0, index, self.plus)
            self.send(self.block(place, 1, index), 1, index, self.minus)

        @pl.when(role == 3)
        def _():
            self.send(self.block(place, 0, index), 4, index, self.minus)

    def send_opposite(self, index):
        self.send(self.block(self.opposite, 0, index), 0, index, self.plus)
        self.send(self.block(self.opposite, 1, index), 1, index, self.minus)

    def send_plus(self, index):
        self.send(self.block(self.plus, 1, index), 3, index, self.plus)

    def send_minus(self, index):
        self.send(self.block(self.minus, 0, index), 4, index, self.minus)

    def forward(self, index):
        self.wait(0, index)
        ref = self.block(self.plus, 0, index)
        add_blocks(ref, (ref, self.landed(0, index)))
        self.send(ref, 2, index, self.plus)
        self.wait(1, index)
        ref = self.block(self.minus, 1, index)
        add_blocks(ref, (ref, self.landed(1, index)))
        self.send(ref, 5, index, self.minus)

    def wait_terms(self, index):
        for kind in (3, 4, 2, 5):
            self.wait(kind, index)

    def terms(self, half, index):
        return (
            self.block(self.here, half, index),
            self.landed(2 + half, index),
            self.landed(4 + half, index),
        )

    def drain(self):
        for kind in range(6):
            self.copies.sent(self.all_landed(kind), self.out + kind, {self.axis: self.plus})


class RowSum:
    def __init__(self, copies, count, blocks, landed):
        self.copies, self.count, self.blocks, self.landed = copies, count, blocks, landed
        self.base, self.out = copies.slots(7 * count), copies.outs(7)
        self.here, self.plus, self.minus, self.opposite = around(X_AXIS)
        self.z = lax.axis_index(Z_AXIS)
        self.other = 1 - self.z

    def send(self, place, half, kind, index, peer):
        slot = self.base + kind * self.count + index
        src = self.blocks.at[place, half, index]
        self.copies.send(src, self.landed.at[kind, index], self.out + kind, slot, peer)

    def wait(self, kind, index):
        slot = self.base + kind * self.count + index
        self.copies.arrived(self.landed.at[kind, index], slot, {Z_AXIS: self.other})

    def send_for(self, place, index):
        role = lax.rem(place - self.here + RING, RING)

        @pl.when(role == 1)
        def _():
            self.send(place, 1, 3, index, {X_AXIS: self.plus})

        @pl.when(role == 2)
        def _():
            self.send(place, 0, 0, index, {X_AXIS: self.plus})
            self.send(place, 1, 1, index, {X_AXIS: self.minus})

        @pl.when(role == 3)
        def _():
            self.send(place, 0, 4, index, {X_AXIS: self.minus})

    def forward(self, index):
        self.wait(0, index)
        ref = self.blocks.at[self.plus, 0, index]
        add_strips(ref, (ref, self.landed.at[0, index]))
        self.send(self.plus, 0, 2, index, {X_AXIS: self.plus})
        self.wait(1, index)
        ref = self.blocks.at[self.minus, 1, index]
        add_strips(ref, (ref, self.landed.at[1, index]))
        self.send(self.minus, 1, 5, index, {X_AXIS: self.minus})

    def terms(self, half, index):
        return (
            self.blocks.at[self.here, half, index],
            self.landed.at[2 + half, index],
            self.landed.at[4 + half, index],
        )

    def pair(self, index):
        for kind in (3, 4, 2, 5):
            self.wait(kind, index)
        add_strips(self.blocks.at[self.here, self.other, index], self.terms(self.other, index))
        self.send(self.here, self.other, 6, index, {Z_AXIS: self.other})

    def finish(self, dst, index):
        self.wait(6, index)
        add_strips(dst, (*self.terms(self.z, index), self.landed.at[6, index]))

    def drain(self):
        for kind in range(7):
            self.copies.sent(self.landed.at[kind], self.out + kind, {Z_AXIS: self.other})


class RowGather:
    def __init__(self, copies, count, buffer):
        self.copies, self.count, self.buffer = copies, count, buffer
        self.base, self.out = copies.slots(7 * count), copies.outs(7)
        self.here, self.plus, self.minus, self.opposite = around(X_AXIS)
        self.z = lax.axis_index(Z_AXIS)
        self.other = 1 - self.z

    def send(self, place, z, kind, index, peer):
        ref = self.buffer.at[place, z, index]
        slot = self.base + kind * self.count + index
        self.copies.send(ref, ref, self.out + kind, slot, peer)

    def wait(self, place, z, kind, index):
        ref = self.buffer.at[place, z, index]
        slot = self.base + kind * self.count + index
        self.copies.arrived(ref, slot, {Z_AXIS: self.other})

    def start(self, index):
        self.send(self.here, self.z, 0, index, {Z_AXIS: self.other})
        self.send(self.here, self.z, 1, index, {X_AXIS: self.plus})
        self.send(self.here, self.z, 2, index, {X_AXIS: self.minus})

    def pair(self, index):
        self.wait(self.here, self.other, 0, index)
        self.send(self.here, self.other, 3, index, {X_AXIS: self.plus})
        self.send(self.here, self.other, 4, index, {X_AXIS: self.minus})

    def forward(self, index):
        self.wait(self.minus, self.z, 1, index)
        self.wait(self.minus, self.other, 3, index)
        self.send(self.minus, 0, 5, index, {X_AXIS: self.plus})
        self.wait(self.plus, self.z, 2, index)
        self.wait(self.plus, self.other, 4, index)
        self.send(self.plus, 1, 6, index, {X_AXIS: self.minus})

    def finish(self, index):
        self.wait(self.opposite, 0, 5, index)
        self.wait(self.opposite, 1, 6, index)

    def drain(self):
        for kind in range(7):
            self.copies.sent(self.buffer.at[0, 0], self.out + kind, {Z_AXIS: self.other})


class RingGather:
    def __init__(self, copies, axis, whole, half, out):
        self.copies, self.axis, self.whole, self.half = copies, axis, whole, half
        self.base, self.out = copies.slots(4), out
        self.here, self.plus, self.minus, self.opposite = around(axis)

    def send(self, ref, kind, peer):
        self.copies.send(ref, ref, self.out + kind, self.base + kind, {self.axis: peer})

    def wait(self, ref, kind):
        self.copies.arrived(ref, self.base + kind, {self.axis: self.plus})

    def start(self):
        self.send(self.whole(self.here), 0, self.plus)
        self.send(self.whole(self.here), 1, self.minus)

    def from_minus(self):
        self.wait(self.whole(self.minus), 0)
        self.send(self.half(self.minus, 0), 2, self.plus)

    def from_plus(self):
        self.wait(self.whole(self.plus), 1)
        self.send(self.half(self.plus, 1), 3, self.minus)

    def forward(self):
        self.from_minus()
        self.from_plus()

    def finish(self):
        self.wait(self.half(self.opposite, 0), 2)
        self.wait(self.half(self.opposite, 1), 3)


class ColGather:
    def __init__(self, copies, buffer):
        here, plus, minus, opposite = around(H_AXIS)
        y = lax.axis_index(Y_AXIS)
        self.copies, self.buffer = copies, buffer
        self.out = copies.outs(8)
        self.outer = RingGather(
            copies,
            H_AXIS,
            lambda place: buffer.at[place, y],
            lambda place, half: buffer.at[place, y, half],
            self.out,
        )
        self.inner = [
            RingGather(
                copies,
                Y_AXIS,
                lambda place, layer=layer: buffer.at[layer, place],
                lambda place, half, layer=layer: buffer.at[layer, place, half],
                self.out + 4,
            )
            for layer in (here, minus, plus, opposite)
        ]
        self.places = (here, minus, plus, opposite)

    def start(self):
        self.outer.start()
        self.inner[0].start()

    def spread(self):
        self.inner[0].forward()

    def outward(self):
        self.outer.from_minus()
        self.inner[1].start()
        self.outer.from_plus()
        self.inner[2].start()

    def first(self, use):
        self.inner[0].finish()
        use(self.places[0])

    def middle(self):
        self.inner[1].forward()
        self.inner[2].forward()
        self.outer.finish()
        self.inner[3].start()

    def second(self, use):
        self.inner[1].finish()
        use(self.places[1])
        self.inner[2].finish()
        use(self.places[2])
        self.inner[3].forward()

    def last(self, use):
        self.inner[3].finish()
        use(self.places[3])

    def drain(self):
        for kind in range(4):
            one = self.buffer.at[0, 0] if kind < 2 else self.buffer.at[0, 0, 0]
            all_layers = self.buffer.at[0] if kind < 2 else self.buffer.at[0, pl.ds(0, 2)]
            self.copies.sent(one, self.out + kind, {H_AXIS: self.outer.plus})
            self.copies.sent(all_layers, self.out + 4 + kind, {H_AXIS: self.outer.plus})


def step_kernel(
    tokens,
    target,
    gate_weight,
    up_weight,
    down_weight,
    probe_gate,
    probe_up,
    probe_down,
    grad_gate_out,
    grad_up_out,
    grad_down_out,
    curv_gate_out,
    curv_up_out,
    curv_down_out,
    sums_out,
    proj,
    down,
    x,
    tgt,
    part,
    part_landed,
    pre,
    hid,
    outs,
    outs_landed,
    layer_sums,
    layer_landed,
    final,
    err,
    back,
    back_landed,
    d_hid,
    coef,
    d_pre,
    grads,
    grads_landed,
    grads_down,
    grads_down_landed,
    tiles,
    tiles_landed,
    results,
    send_sems,
    recv_sems,
    out_sems,
):
    copies = Copies(send_sems, recv_sems)
    core = lax.axis_index(CORE_AXIS)
    other_core = 1 - core
    x_here, x_plus, x_minus, x_opposite = around(X_AXIS)
    y_here, y_plus, y_minus, y_opposite = around(Y_AXIS)
    h_here, h_plus, h_minus, h_opposite = around(H_AXIS)
    z_here = lax.axis_index(Z_AXIS)
    partner = {CORE_AXIS: other_core}

    barrier = pltpu.get_barrier_semaphore()
    z_other = 1 - z_here
    peers = [partner, {Z_AXIS: z_other}]
    for axis in (X_AXIS, Y_AXIS, H_AXIS):
        peers += [{axis: place} for place in around(axis)[1:]]
    for peer in peers:
        pl.semaphore_signal(barrier, inc=1, device_id=peer, device_id_type=MESH)

    own_rows = pl.ds(pl.multiple_of(core * HALF, HALF), HALF)
    other_rows = pl.ds(pl.multiple_of(other_core * HALF, HALF), HALF)
    x[h_here, y_here, core] = tokens[own_rows, :]
    tgt[core] = target[own_rows, :]

    def sign(ref):
        return (2 * ref[...] - 1).astype(F32).astype(BF16)

    def lay_out(dst, index, values):
        dst[core, index, PADDED - 32 :] = jnp.zeros((32, FEATS), BF16)
        dst[core, index, :UNITS] = values

    lay_out(proj, 0, gate_weight[...])
    lay_out(proj, 1, up_weight[...])
    lay_out(proj, 2, sign(probe_gate))
    lay_out(proj, 3, sign(probe_up))
    lay_out(down, 0, down_weight[...])
    lay_out(down, 1, sign(probe_down))

    pl.semaphore_wait(barrier, len(peers))
    near = copies.slots(9)
    copies.outs(9)
    copies.send(tokens.at[other_rows], x.at[h_here, y_here, core], near, near, partner)
    copies.send(proj.at[core], proj.at[core], near + 1, near + 1, partner)
    copies.send(target.at[other_rows], tgt.at[core], near + 2, near + 2, partner)
    copies.send(down.at[core], down.at[core], near + 3, near + 3, partner)

    copies.arrived(x.at[h_here, y_here, other_core], near, partner)
    x_gather = ColGather(copies, x)
    x_gather.start()
    x_gather.spread()
    x_gather.outward()

    def token_block(ref, *place):
        return [
            ref[(*place, slice(None), half)].reshape(RING * HALF, FEATS) for half in range(2)
        ]

    row_sum = RowSum(copies, 4, part, part_landed)

    def project(index, place):
        left, right = token_block(x, place)
        both = dot_nt(proj[0, index], left) + dot_nt(proj[1, index], right)
        both = both.astype(BF16)
        part[place, 0, index] = both[:, :LANES]
        part[place, 1, index] = both[:, LANES:]

    def each(count, step):
        def body(index, carry):
            step(index)
            return carry

        lax.fori_loop(0, count, body, 0)

    def project_and_send(place):
        def one(index):
            project(index, place)
            row_sum.send_for(place, index)

        each(4, one)

    def project_first(place):
        copies.arrived(proj.at[other_core], near + 1, partner)
        project_and_send(place)

    x_gather.first(project_first)
    x_gather.middle()
    x_gather.second(project_and_send)
    x_gather.last(project_and_send)
    each(4, row_sum.forward)
    each(4, row_sum.pair)

    def strips(step):
        def body(index, carry):
            step(pl.ds(pl.multiple_of(index * STRIP, STRIP), STRIP))
            return carry

        lax.fori_loop(0, PADDED // STRIP, body, 0)

    def hide(rows):
        pre_gate, pre_up = pre[0, rows, :], pre[1, rows, :]
        act = pre_gate * jax.nn.sigmoid(pre_gate)
        hid[x_here, z_here, 0, rows, :] = (act * pre_up).astype(BF16)

    def hide_dot(rows):
        pre_gate, pre_up = pre[0, rows, :], pre[1, rows, :]
        dot_gate, dot_up = pre[2, rows, :], pre[3, rows, :]
        sig = jax.nn.sigmoid(pre_gate)
        act = pre_gate * sig
        slope = sig * (1.0 + pre_gate * (1.0 - sig))
        bend = sig * (1.0 - sig) * (2.0 + pre_gate * (1.0 - 2.0 * sig))
        hid[x_here, z_here, 1, rows, :] = (slope * dot_gate * pre_up + act * dot_up).astype(BF16)
        coef[x_here, z_here, 0, rows, :] = (pre_up * slope).astype(BF16)
        coef[x_here, z_here, 1, rows, :] = act.astype(BF16)
        coef[x_here, z_here, 2, rows, :] = (dot_up * slope + pre_up * bend * dot_gate).astype(BF16)
        coef[x_here, z_here, 3, rows, :] = (slope * dot_gate).astype(BF16)

    hid_gather = RowGather(copies, 2, hid)
    each(2, lambda index: row_sum.finish(pre.at[index], index))
    strips(hide)
    hid_gather.start(0)
    each(2, lambda index: row_sum.finish(pre.at[2 + index], 2 + index))
    strips(hide_dot)
    hid_gather.start(1)
    layers = [(0, x_here), (1, x_minus), (2, x_plus), (3, x_opposite)]

    def out_ring(stream):
        return RingSum(
            copies,
            Y_AXIS,
            4,
            lambda place, half, layer: outs.at[stream, layer[1], place, half],
            lambda kind, layer: outs_landed.at[stream, kind, layer[0]],
            lambda kind: outs_landed.at[stream, kind],
            lambda layer: layer[0],
        )

    def layer_ring(stream):
        return RingSum(
            copies,
            H_AXIS,
            1,
            lambda place, half, index: layer_sums.at[stream, place, half],
            lambda kind, index: layer_landed.at[stream, kind],
            lambda kind: layer_landed.at[stream, kind],
        )

    out_sums = (out_ring(0), out_ring(1))
    layer_rings = (layer_ring(0), layer_ring(1))
    err_gathers = (ColGather(copies, err.at[0]), ColGather(copies, err.at[1]))
    back_sum = RowSum(copies, 2, back, back_landed)
    coef_gather = RowGather(copies, 4, coef)
    back_gather = RowGather(copies, 2, d_hid)

    def whole_units(ref, place, index):
        return jnp.concatenate([ref[place, 0, index], ref[place, 1, index]], axis=1)

    def expand(stream, layer):
        place = layer[1]
        plain = whole_units(hid, place, 0)
        for half in range(2):
            if stream == 0:
                value = dot_tn(plain, down[half, 0])
            else:
                tangent = whole_units(hid, place, 1)
                value = dot_tn(tangent, down[half, 0]) + dot_tn(plain, down[half, 1])
            value = value.astype(BF16).reshape(RING, HALF, FEATS)
            for block in range(RING):
                outs[stream, place, block, half] = value[block]
        out_sums[stream].send_opposite(layer)
        out_sums[stream].send_plus(layer)
        out_sums[stream].send_minus(layer)

    def complete(stream, layer):
        out_sum = out_sums[stream]
        out_sum.wait_terms(layer)
        for half in range(2):
            add_blocks(layer_sums.at[stream, layer[1], half], out_sum.terms(half, layer))
        layer_rings[stream].send_for(layer[1], 0)

    def settle(stream):
        ring = layer_rings[stream]
        ring.wait_terms(0)
        for half in range(2):
            add_blocks(final.at[half], ring.terms(half, 0))
            value = final[half]
            if stream == 0:
                value = value - tgt[half].astype(F32)
            err[stream, h_here, y_here, half] = value.astype(BF16)
        err_gathers[stream].start()

    def turn_back(stream):
        def one(place):
            plain = token_block(err, 0, place)
            if stream == 0:
                whole = dot_nt(down[0, 0], plain[0]) + dot_nt(down[1, 0], plain[1])
            else:
                tangent = token_block(err, 1, place)
                whole = dot_nt(down[0, 0], tangent[0]) + dot_nt(down[1, 0], tangent[1])
                whole = whole + dot_nt(down[0, 1], plain[0]) + dot_nt(down[1, 1], plain[1])
            whole = whole.astype(BF16)
            back[place, 0, stream] = whole[:, :LANES]
            back[place, 1, stream] = whole[:, LANES:]
            back_sum.send_for(place, stream)

        return one

    def slopes(place):
        for z in range(2):

            def one(rows):
                d_hidden = d_hid[place, z, 0, rows, :].astype(F32)
                for index in range(2):
                    factor = coef[place, z, index, rows, :].astype(F32)
                    d_pre[place, z, index, rows, :] = (d_hidden * factor).astype(BF16)

            strips(one)

    def bends(place):
        for z in range(2):

            def one(rows):
                d_hidden = d_hid[place, z, 0, rows, :].astype(F32)
                d_hidden_dot = d_hid[place, z, 1, rows, :].astype(F32)
                for index in range(2):
                    factor = coef[place, z, index, rows, :].astype(F32)
                    bent = coef[place, z, 2 + index, rows, :].astype(F32)
                    value = d_hidden_dot * factor + d_hidden * bent
                    d_pre[place, z, 2 + index, rows, :] = value.astype(BF16)

            strips(one)

    hid_gather.pair(0)
    copies.arrived(down.at[other_core], near + 3, partner)
    expand(0, layers[0])
    hid_gather.forward(0)
    expand(0, layers[1])
    expand(0, layers[2])
    hid_gather.pair(1)
    expand(1, layers[0])
    out_sums[0].forward(layers[0])
    hid_gather.forward(1)
    expand(1, layers[1])
    expand(1, layers[2])
    each(4, coef_gather.start)
    hid_gather.finish(0)
    expand(0, layers[3])
    complete(0, layers[0])
    out_sums[0].forward(layers[1])
    out_sums[0].forward(layers[2])
    out_sums[1].forward(layers[0])
    hid_gather.finish(1)
    expand(1, layers[3])
    out_sums[0].forward(layers[3])
    complete(0, layers[1])
    complete(0, layers[2])
    complete(1, layers[0])
    out_sums[1].forward(layers[1])
    out_sums[1].forward(layers[2])
    complete(0, layers[3])
    each(4, coef_gather.pair)
    layer_rings[0].forward(0)
    out_sums[1].forward(layers[3])
    complete(1, layers[1])
    complete(1, layers[2])
    copies.arrived(tgt.at[other_core], near + 2, partner)
    settle(0)
    complete(1, layers[3])
    layer_rings[1].forward(0)
    err_gathers[0].spread()
    err_gathers[0].outward()
    settle(1)
    each(4, coef_gather.forward)
    err_gathers[0].first(turn_back(0))
    err_gathers[0].middle()
    err_gathers[1].spread()
    err_gathers[1].outward()
    err_gathers[0].second(turn_back(0))
    err_gathers[1].first(turn_back(1))
    err_gathers[1].middle()
    err_gathers[0].last(turn_back(0))
    err_gathers[1].second(turn_back(1))
    back_sum.forward(0)
    err_gathers[1].last(turn_back(1))
    back_sum.pair(0)
    back_sum.forward(1)
    back_sum.finish(d_hid.at[x_here, z_here, 0], 0)
    back_gather.start(0)
    back_sum.pair(1)
    back_gather.pair(0)
    back_sum.finish(d_hid.at[x_here, z_here, 1], 1)
    back_gather.start(1)
    back_gather.forward(0)
    back_gather.pair(1)
    each(4, coef_gather.finish)

    def down_grads(side):
        plain_sum = jnp.zeros((PADDED, FEATS), F32)
        along_sum = jnp.zeros((PADDED, FEATS), F32)
        for place in range(RING):
            plain = whole_units(hid, place, 0)
            tangent = whole_units(hid, place, 1)
            err_block = err[0, place, :, side].reshape(RING * HALF, FEATS)
            dot_block = err[1, place, :, side].reshape(RING * HALF, FEATS)
            plain_sum = plain_sum + dot_nn(plain, err_block)
            along_sum = along_sum + dot_nn(tangent, err_block) + dot_nn(plain, dot_block)
        grads_down[side, 0] = plain_sum
        grads_down[side, 1] = along_sum

    down_grads(other_core)
    copies.send(grads_down.at[other_core], grads_down_landed, near + 4, near + 4, partner)
    down_grads(core)

    def tokens_of(place, side):
        return x[place, :, side].reshape(RING * HALF, FEATS)

    def first_grads(side, index):
        total = dot_nn(whole_units(d_pre, x_here, index), tokens_of(x_here, side))
        for place in (x_minus, x_plus):
            total = total + dot_nn(whole_units(d_pre, place, index), tokens_of(place, side))
        grads[side, index] = total

    def last_grads(side, index):
        last = dot_nn(whole_units(d_pre, x_opposite, index), tokens_of(x_opposite, side))
        grads[side, index] = grads[side, index] + last

    def last_and_send(index):
        last_grads(other_core, index)
        copies.send(grads.at[other_core, index], grads_landed.at[index], near + 5 + index, near + 5 + index, partner)
        last_grads(core, index)

    def first_both(index):
        first_grads(other_core, index)
        first_grads(core, index)

    def squares(values):
        return jnp.sum(values * values, axis=0, keepdims=True)

    outputs = (grad_gate_out, grad_up_out, grad_down_out, curv_gate_out, curv_up_out, curv_down_out)

    def to_output(index):
        return pltpu.make_async_copy(results.at[index], outputs[index], out_sems.at[index])

    def give(index, values):
        results[index] = values[:UNITS]
        to_output(index).start()

    for place in (x_here, x_minus, x_plus):
        slopes(place)
    each(2, first_both)
    back_gather.forward(1)
    back_gather.finish(0)
    slopes(x_opposite)
    each(2, last_and_send)
    for place in (x_here, x_minus, x_plus):
        bends(place)
    each(2, lambda index: first_both(2 + index))
    back_gather.finish(1)
    bends(x_opposite)
    each(2, lambda index: last_and_send(2 + index))

    copies.arrived(grads_down_landed, near + 4, partner)
    grad = grads_down[core, 0] + grads_down_landed[0]
    hess = grads_down[core, 1] + grads_down_landed[1]
    give(2, grad)
    grad_sum = squares(grad)
    curv = curvature(down[core, 1].astype(F32), hess)
    give(5, curv)
    curv_sum = squares(curv)

    for index in range(2):
        copies.arrived(grads_landed.at[index], near + 5 + index, partner)
        grad = grads[core, index] + grads_landed[index]
        give(index, grad)
        grad_sum = grad_sum + squares(grad)
    for index in range(2):
        copies.arrived(grads_landed.at[2 + index], near + 7 + index, partner)
        hess = grads[core, 2 + index] + grads_landed[2 + index]
        curv = curvature(proj[core, 2 + index].astype(F32), hess)
        give(3 + index, curv)
        curv_sum = curv_sum + squares(curv)

    lane = lax.broadcasted_iota(jnp.int32, (8, LANES), 1)
    grad_sum = jnp.sum(grad_sum, axis=1, keepdims=True)
    curv_sum = jnp.sum(curv_sum, axis=1, keepdims=True)
    tiles[0] = jnp.where(lane == 0, grad_sum, jnp.where(lane == 1, curv_sum, 0.0))

    stages = [
        [partner],
        [{Z_AXIS: z_other}],
        [{X_AXIS: x_plus}, {X_AXIS: x_opposite}, {X_AXIS: x_minus}],
        [{Y_AXIS: y_plus}, {Y_AXIS: y_opposite}, {Y_AXIS: y_minus}],
        [{H_AXIS: h_plus}, {H_AXIS: h_opposite}, {H_AXIS: h_minus}],
    ]
    small = copies.slots(3 * len(stages))
    small_out = copies.outs(3 * len(stages))
    for stage, receivers in enumerate(stages):
        for index, peer in enumerate(receivers):
            slot = 3 * stage + index
            landed = tiles_landed.at[stage, index]
            copies.send(tiles.at[stage], landed, small_out + slot, small + slot, peer)
        total = tiles[stage]
        for index, peer in enumerate(receivers):
            copies.arrived(tiles_landed.at[stage, index], small + 3 * stage + index, peer)
            total = total + tiles_landed[stage, index]
        tiles[stage + 1] = total
    sums_out[...] = tiles[len(stages)]

    assert (copies.next_out, copies.next_in) == (SENDS, ARRIVALS), (copies.next_out, copies.next_in)
    for index in range(len(outputs)):
        to_output(index).wait()
    copies.sent(x.at[0, 0, 0], near, partner)
    copies.sent(proj.at[0], near + 1, partner)
    copies.sent(tgt.at[0], near + 2, partner)
    copies.sent(down.at[0], near + 3, partner)
    copies.sent(grads_down_landed, near + 4, partner)
    each(4, lambda index: copies.sent(grads_landed.at[index], near + 5 + index, partner))
    x_gather.drain()
    err_gathers[0].drain()
    err_gathers[1].drain()
    row_sum.drain()
    back_sum.drain()
    hid_gather.drain()
    coef_gather.drain()
    back_gather.drain()
    for stream in range(2):
        out_sums[stream].drain()
        layer_rings[stream].drain()
    for stage, receivers in enumerate(stages):
        for index, peer in enumerate(receivers):
            copies.sent(tiles.at[stage], small_out + 3 * stage + index, peer)


SENDS = 107
ARRIVALS = 242


def whole_step(*operands):
    units = (PADDED, LANES)
    block = (2, HALF, FEATS)
    return pl.pallas_call(
        step_kernel,
        out_shape=(
            *[jax.ShapeDtypeStruct((UNITS, FEATS), F32)] * 6,
            jax.ShapeDtypeStruct((8, LANES), F32),
        ),
        in_specs=[pl.BlockSpec(memory_space=pltpu.VMEM)] * 8,
        out_specs=[pl.BlockSpec(memory_space=pl.ANY)] * 6 + [pl.BlockSpec(memory_space=pltpu.VMEM)],
        scratch_shapes=[
            pltpu.VMEM((2, 4, PADDED, FEATS), BF16),
            pltpu.VMEM((2, 2, PADDED, FEATS), BF16),
            pltpu.VMEM((RING, RING, *block), BF16),
            pltpu.VMEM(block, BF16),
            pltpu.VMEM((RING, 2, 4, *units), BF16),
            pltpu.VMEM((7, 4, *units), BF16),
            pltpu.VMEM((4, *units), F32),
            pltpu.VMEM((RING, 2, 2, *units), BF16),
            pltpu.VMEM((2, RING, RING, *block), BF16),
            pltpu.VMEM((2, 6, RING, HALF, FEATS), BF16),
            pltpu.VMEM((2, RING, *block), BF16),
            pltpu.VMEM((2, 6, HALF, FEATS), BF16),
            pltpu.VMEM(block, F32),
            pltpu.VMEM((2, RING, RING, *block), BF16),
            pltpu.VMEM((RING, 2, 2, *units), BF16),
            pltpu.VMEM((7, 2, *units), BF16),
            pltpu.VMEM((RING, 2, 2, *units), BF16),
            pltpu.VMEM((RING, 2, 4, *units), BF16),
            pltpu.VMEM((RING, 2, 4, *units), BF16),
            pltpu.VMEM((2, 4, PADDED, FEATS), F32),
            pltpu.VMEM((4, PADDED, FEATS), F32),
            pltpu.VMEM((2, 2, PADDED, FEATS), F32),
            pltpu.VMEM((2, PADDED, FEATS), F32),
            pltpu.VMEM((6, 8, LANES), F32),
            pltpu.VMEM((5, 3, 8, LANES), F32),
            pltpu.VMEM((6, UNITS, FEATS), F32),
            pltpu.SemaphoreType.DMA((SENDS,)),
            pltpu.SemaphoreType.DMA((ARRIVALS,)),
            pltpu.SemaphoreType.DMA((6,)),
        ],
        compiler_params=pltpu.CompilerParams(
            collective_id=0, has_side_effects=True, vmem_limit_bytes=60 * 1024 * 1024
        ),
    )(*operands)


def update_kernel(sums, *refs):
    count = 3.0 * D * FF
    rms_grad = jnp.sqrt(sums[0:1, 0:1] / count + 1e-06)
    rms_curv = jnp.sqrt(sums[0:1, 1:2] / count + 1e-06)
    fix_first = 1.0 - 0.9**STEP
    fix_second = 1.0 - 0.95**STEP
    for weight in range(3):
        grad, curv, first, second, first_out, second_out, update_out = refs[weight::3]
        new_first = 0.9 * first[...] + 0.1 * (grad[...] / rms_grad)
        scaled = curv[...] / rms_curv
        new_second = 0.95 * second[...] + 0.05 * (scaled * scaled)
        first_out[...] = new_first
        second_out[...] = new_second
        update_out[...] = new_first / fix_first / (jnp.sqrt(new_second / fix_second) + 1e-08)


def update(sums, *arrays):
    rows = pl.BlockSpec((88, FEATS), lambda step: (step, 0))
    return pl.pallas_call(
        update_kernel,
        out_shape=[jax.ShapeDtypeStruct((UNITS, FEATS), F32)] * 9,
        grid=(4,),
        in_specs=[pl.BlockSpec((8, LANES), lambda step: (0, 0))] + [rows] * 12,
        out_specs=[rows] * 9,
    )(sums, *arrays)


def body(
    tokens,
    target,
    gate_weight,
    up_weight,
    down_weight,
    probe_gate,
    probe_up,
    probe_down,
    first_gate,
    first_up,
    first_down,
    second_gate,
    second_up,
    second_down,
):
    *arrays, sums = whole_step(
        tokens, target, gate_weight.T, up_weight.T, down_weight, probe_gate.T, probe_up.T, probe_down
    )
    outs = update(
        sums, *arrays, first_gate.T, first_up.T, first_down, second_gate.T, second_up.T, second_down
    )
    return tuple(value if index % 3 == 2 else value.T for index, value in enumerate(outs))


def solution(mesh):
    torus = Mesh(mesh.devices.reshape(4, 2, 2, 4, 4), (*ROW, *COL))
    feats, units = P(ROW, COL), P(COL, ROW)
    in_specs = (units, units, feats, feats, units) + (feats, feats, units) * 3
    out_specs = (feats, feats, units) * 3
    return jax.shard_map(body, mesh=torus, in_specs=in_specs, out_specs=out_specs, check_vma=False)
```

```python
import jax
import jax.numpy as jnp
from jax import lax
from jax.experimental import pallas as pl
from jax.experimental.pallas import tpu as pltpu
from jax.sharding import Mesh
from jax.sharding import PartitionSpec as P

D = 4096
FF = 5504
STEP = 10
COL = ("col_0", "col_1")
ROW = ("row_0", "row_1", "row_2")
RING = 4
UNITS = 344
PADDED = 352
FEATS = 256
HALF = 64
LANES = 128
STRIP = 32
MESH = pl.DeviceIdType.MESH
BF16 = jnp.bfloat16
F32 = jnp.float32

X_AXIS, Z_AXIS, CORE_AXIS = ROW
H_AXIS, Y_AXIS = COL


def dot_nn(left, right):
    return jnp.dot(left, right, preferred_element_type=F32)


def dot_nt(left, right):
    return lax.dot_general(left, right, (((1,), (1,)), ((), ())), preferred_element_type=F32)


def dot_tn(left, right):
    return lax.dot_general(left, right, (((0,), (0,)), ((), ())), preferred_element_type=F32)


def block_ones(size):
    rows = lax.broadcasted_iota(jnp.int32, (size, size), 0) >> 2
    cols = lax.broadcasted_iota(jnp.int32, (size, size), 1) >> 2
    return jnp.where(rows == cols, 1.0, 0.0).astype(BF16)


def two_terms(values):
    high = values.astype(BF16)
    low = (values - high.astype(F32)).astype(BF16)
    return high, low


def curvature(sign, hess):
    high, low = two_terms(jnp.abs(sign * hess))
    ones = block_ones(hess.shape[0])
    down = dot_nn(ones, high) + dot_nn(ones, low)
    high, low = two_terms(down)
    ones = block_ones(hess.shape[1])
    return (dot_nn(high, ones) + dot_nn(low, ones)) * 0.0625


class Copies:
    def __init__(self, send_sems, recv_sems):
        self.send_sems = send_sems
        self.recv_sems = recv_sems
        self.next_in = 0
        self.next_out = 0

    def slots(self, count):
        self.next_in += count
        return self.next_in - count

    def outs(self, count):
        self.next_out += count
        return self.next_out - count

    def copy(self, src, dst, out, slot, peer):
        return pltpu.make_async_remote_copy(
            src_ref=src,
            dst_ref=dst,
            send_sem=self.send_sems.at[out],
            recv_sem=self.recv_sems.at[slot],
            device_id=peer,
            device_id_type=MESH,
        )

    def send(self, src, dst, out, slot, peer):
        self.copy(src, dst, out, slot, peer).start()

    def arrived(self, dst, slot, peer):
        self.copy(dst, dst, 0, slot, peer).wait_recv()

    def sent(self, src, out, peer):
        self.copy(src, src, out, 0, peer).wait_send()


def around(axis):
    here = lax.axis_index(axis)
    return here, lax.rem(here + 1, RING), lax.rem(here + 3, RING), lax.rem(here + 2, RING)


def add_strips(dst, terms):
    def strip(index, carry):
        rows = pl.ds(pl.multiple_of(index * STRIP, STRIP), STRIP)
        total = terms[0][rows, :].astype(F32)
        for term in terms[1:]:
            total = total + term[rows, :].astype(F32)
        dst[rows, :] = total.astype(dst.dtype)
        return carry

    lax.fori_loop(0, PADDED // STRIP, strip, 0)


def add_blocks(dst, terms):
    total = terms[0][...].astype(F32)
    for term in terms[1:]:
        total = total + term[...].astype(F32)
    dst[...] = total.astype(dst.dtype)


class RingSum:
    def __init__(self, copies, axis, count, block, landed, all_landed, last, number=lambda index: index):
        self.last = last
        self.number, self.all_landed = number, all_landed
        self.out = copies.outs(6)
        self.copies, self.axis, self.block, self.landed = copies, axis, block, landed
        self.base = copies.slots(3 * count)
        self.count = count
        self.here, self.plus, self.minus, self.opposite = around(axis)

    def slot(self, kind, index):
        return self.base + min(kind, 2) * self.count + self.number(index)

    def send(self, src, kind, index, peer):
        slot = self.slot(kind, index)
        self.copies.send(src, self.landed(kind, index), self.out + kind, slot, {self.axis: peer})

    def wait(self, kind, index):
        ref = self.landed(kind, index)
        self.copies.arrived(ref, self.slot(kind, index), {self.axis: self.plus})

    def send_for(self, place, index):
        role = lax.rem(place - self.here + RING, RING)

        @pl.when(role == 1)
        def _():
            self.send(self.block(place, 1, index), 3, index, self.plus)

        @pl.when(role == 2)
        def _():
            self.send(self.block(place, 0, index), 0, index, self.plus)
            self.send(self.block(place, 1, index), 1, index, self.minus)

        @pl.when(role == 3)
        def _():
            self.send(self.block(place, 0, index), 4, index, self.minus)

    def send_opposite(self, index):
        self.send(self.block(self.opposite, 0, index), 0, index, self.plus)
        self.send(self.block(self.opposite, 1, index), 1, index, self.minus)

    def send_plus(self, index):
        self.send(self.block(self.plus, 1, index), 3, index, self.plus)

    def send_minus(self, index):
        self.send(self.block(self.minus, 0, index), 4, index, self.minus)

    def forward(self, index):
        self.wait(0, index)
        ref = self.block(self.plus, 0, index)
        add_blocks(ref, (ref, self.landed(0, index)))
        self.send(ref, 2, index, self.plus)
        self.wait(1, index)
        ref = self.block(self.minus, 1, index)
        add_blocks(ref, (ref, self.landed(1, index)))
        self.send(ref, 5, index, self.minus)

    def wait_terms(self, index):
        self.copies.arrived(self.last(index), self.slot(2, index), {self.axis: self.plus})

    def terms(self, half, index):
        return (
            self.block(self.here, half, index),
            self.landed(2 + half, index),
            self.landed(4 + half, index),
        )

    def drain(self):
        for kind in range(6):
            self.copies.sent(self.all_landed(kind), self.out + kind, {self.axis: self.plus})


class RowSum:
    def __init__(self, copies, count, blocks, landed):
        self.copies, self.count, self.blocks, self.landed = copies, count, blocks, landed
        self.base, self.out = copies.slots(4 * count), copies.outs(7)
        self.here, self.plus, self.minus, self.opposite = around(X_AXIS)
        self.z = lax.axis_index(Z_AXIS)
        self.other = 1 - self.z

    def slot(self, kind, index):
        return self.base + (0, 1, 2, 2, 2, 2, 3)[kind] * self.count + index

    def send(self, place, half, kind, index, peer):
        src = self.blocks.at[place, half, index]
        slot = self.slot(kind, index)
        self.copies.send(src, self.landed.at[kind, index], self.out + kind, slot, peer)

    def wait(self, kind, index):
        ref = self.landed.at[pl.ds(2, 4) if kind == 2 else kind, index]
        self.copies.arrived(ref, self.slot(kind, index), {Z_AXIS: self.other})

    def send_for(self, place, index):
        role = lax.rem(place - self.here + RING, RING)

        @pl.when(role == 1)
        def _():
            self.send(place, 1, 3, index, {X_AXIS: self.plus})

        @pl.when(role == 2)
        def _():
            self.send(place, 0, 0, index, {X_AXIS: self.plus})
            self.send(place, 1, 1, index, {X_AXIS: self.minus})

        @pl.when(role == 3)
        def _():
            self.send(place, 0, 4, index, {X_AXIS: self.minus})

    def forward(self, index):
        self.wait(0, index)
        ref = self.blocks.at[self.plus, 0, index]
        add_strips(ref, (ref, self.landed.at[0, index]))
        self.send(self.plus, 0, 2, index, {X_AXIS: self.plus})
        self.wait(1, index)
        ref = self.blocks.at[self.minus, 1, index]
        add_strips(ref, (ref, self.landed.at[1, index]))
        self.send(self.minus, 1, 5, index, {X_AXIS: self.minus})

    def terms(self, half, index):
        return (
            self.blocks.at[self.here, half, index],
            self.landed.at[2 + half, index],
            self.landed.at[4 + half, index],
        )

    def pair(self, index):
        self.wait(2, index)
        add_strips(self.blocks.at[self.here, self.other, index], self.terms(self.other, index))
        self.send(self.here, self.other, 6, index, {Z_AXIS: self.other})

    def finish(self, dst, index):
        self.wait(6, index)
        add_strips(dst, (*self.terms(self.z, index), self.landed.at[6, index]))

    def drain(self):
        for kind in range(7):
            self.copies.sent(self.landed.at[kind], self.out + kind, {Z_AXIS: self.other})


class RowGather:
    def __init__(self, copies, count, buffer):
        self.copies, self.count, self.buffer = copies, count, buffer
        self.base, self.out = copies.slots(7 * count), copies.outs(7)
        self.here, self.plus, self.minus, self.opposite = around(X_AXIS)
        self.z = lax.axis_index(Z_AXIS)
        self.other = 1 - self.z

    def send(self, place, z, kind, index, peer):
        ref = self.buffer.at[place, z, index]
        slot = self.base + kind * self.count + index
        self.copies.send(ref, ref, self.out + kind, slot, peer)

    def wait(self, place, z, kind, index):
        ref = self.buffer.at[place, z, index]
        slot = self.base + kind * self.count + index
        self.copies.arrived(ref, slot, {Z_AXIS: self.other})

    def start(self, index):
        self.start_pair(index)
        self.start_ring(index)

    def start_pair(self, index):
        self.send(self.here, self.z, 0, index, {Z_AXIS: self.other})

    def start_ring(self, index):
        self.send(self.here, self.z, 1, index, {X_AXIS: self.plus})
        self.send(self.here, self.z, 2, index, {X_AXIS: self.minus})

    def pair(self, index):
        self.wait(self.here, self.other, 0, index)
        self.send(self.here, self.other, 3, index, {X_AXIS: self.plus})
        self.send(self.here, self.other, 4, index, {X_AXIS: self.minus})

    def forward(self, index):
        self.wait(self.minus, self.z, 1, index)
        self.wait(self.minus, self.other, 3, index)
        self.send(self.minus, 0, 5, index, {X_AXIS: self.plus})
        self.wait(self.plus, self.z, 2, index)
        self.wait(self.plus, self.other, 4, index)
        self.send(self.plus, 1, 6, index, {X_AXIS: self.minus})

    def finish(self, index):
        self.wait(self.opposite, 0, 5, index)
        self.wait(self.opposite, 1, 6, index)

    def drain(self):
        for kind in range(7):
            self.copies.sent(self.buffer.at[0, 0], self.out + kind, {Z_AXIS: self.other})


class RingGather:
    def __init__(self, copies, axis, whole, half, out):
        self.copies, self.axis, self.whole, self.half = copies, axis, whole, half
        self.base, self.out = copies.slots(4), out
        self.here, self.plus, self.minus, self.opposite = around(axis)

    def send(self, ref, kind, peer):
        self.copies.send(ref, ref, self.out + kind, self.base + kind, {self.axis: peer})

    def wait(self, ref, kind):
        self.copies.arrived(ref, self.base + kind, {self.axis: self.plus})

    def start(self):
        self.send(self.whole(self.here), 0, self.plus)
        self.send(self.whole(self.here), 1, self.minus)

    def from_minus(self):
        self.wait(self.whole(self.minus), 0)
        self.send(self.half(self.minus, 0), 2, self.plus)

    def from_plus(self):
        self.wait(self.whole(self.plus), 1)
        self.send(self.half(self.plus, 1), 3, self.minus)

    def forward(self):
        self.from_minus()
        self.from_plus()

    def finish(self):
        self.wait(self.half(self.opposite, 0), 2)
        self.wait(self.half(self.opposite, 1), 3)


class ColGather:
    def __init__(self, copies, buffer):
        here, plus, minus, opposite = around(H_AXIS)
        y = lax.axis_index(Y_AXIS)
        self.copies, self.buffer = copies, buffer
        self.out = copies.outs(8)
        self.outer = RingGather(
            copies,
            H_AXIS,
            lambda place: buffer.at[place, y],
            lambda place, half: buffer.at[place, y, half],
            self.out,
        )
        self.inner = [
            RingGather(
                copies,
                Y_AXIS,
                lambda place, layer=layer: buffer.at[layer, place],
                lambda place, half, layer=layer: buffer.at[layer, place, half],
                self.out + 4,
            )
            for layer in (here, minus, plus, opposite)
        ]
        self.places = (here, minus, plus, opposite)

    def start(self):
        self.outer.start()
        self.inner[0].start()

    def spread(self):
        self.inner[0].forward()

    def outward(self):
        self.outer.from_minus()
        self.inner[1].start()
        self.outer.from_plus()
        self.inner[2].start()

    def first(self, use):
        self.inner[0].finish()
        use(self.places[0])

    def middle(self):
        self.inner[1].forward()
        self.inner[2].forward()
        self.outer.finish()
        self.inner[3].start()

    def second(self, use):
        self.inner[1].finish()
        use(self.places[1])
        self.inner[2].finish()
        use(self.places[2])
        self.inner[3].forward()

    def last(self, use):
        self.inner[3].finish()
        use(self.places[3])

    def drain(self):
        for kind in range(4):
            one = self.buffer.at[0, 0] if kind < 2 else self.buffer.at[0, 0, 0]
            all_layers = self.buffer.at[0] if kind < 2 else self.buffer.at[0, pl.ds(0, 2)]
            self.copies.sent(one, self.out + kind, {H_AXIS: self.outer.plus})
            self.copies.sent(all_layers, self.out + 4 + kind, {H_AXIS: self.outer.plus})


def step_kernel(
    tokens,
    target,
    gate_weight,
    up_weight,
    down_weight,
    probe_gate,
    probe_up,
    probe_down,
    grad_gate_out,
    grad_up_out,
    grad_down_out,
    curv_gate_out,
    curv_up_out,
    curv_down_out,
    sums_out,
    proj,
    down,
    x,
    tgt,
    part,
    part_landed,
    pre,
    hid,
    outs,
    outs_landed,
    layer_sums,
    layer_landed,
    final,
    err,
    back,
    back_landed,
    d_hid,
    coef,
    d_pre,
    grads,
    grads_landed,
    grads_down,
    grads_down_landed,
    tiles,
    tiles_landed,
    results,
    send_sems,
    recv_sems,
    out_sems,
):
    copies = Copies(send_sems, recv_sems)
    core = lax.axis_index(CORE_AXIS)
    other_core = 1 - core
    x_here, x_plus, x_minus, x_opposite = around(X_AXIS)
    y_here, y_plus, y_minus, y_opposite = around(Y_AXIS)
    h_here, h_plus, h_minus, h_opposite = around(H_AXIS)
    z_here = lax.axis_index(Z_AXIS)
    partner = {CORE_AXIS: other_core}

    barrier = pltpu.get_barrier_semaphore()
    def displaced(axes, sizes):
        steps = [()]
        for size in sizes:
            steps = [(*step, more) for step in steps for more in range(size)]
        return [
            {
                axis: lax.rem(lax.axis_index(axis) + more, size)
                for axis, size, more in zip(axes, sizes, step)
            }
            for step in steps[1:]
        ]

    row_peers = displaced(ROW, (RING, 2, 2))
    col_peers = displaced(COL, (RING, RING))
    peers = row_peers + col_peers
    for peer in peers:
        pl.semaphore_signal(barrier, inc=1, device_id=peer, device_id_type=MESH)

    own_rows = pl.ds(pl.multiple_of(core * HALF, HALF), HALF)
    other_rows = pl.ds(pl.multiple_of(other_core * HALF, HALF), HALF)
    x[h_here, y_here, core] = tokens[own_rows, :]
    tgt[core] = target[own_rows, :]

    def sign(ref):
        return (2 * ref[...] - 1).astype(F32).astype(BF16)

    def lay_out(dst, index, values):
        dst[core, index, PADDED - 32 :] = jnp.zeros((32, FEATS), BF16)
        dst[core, index, :UNITS] = values

    lay_out(proj, 0, gate_weight[...])
    lay_out(proj, 1, up_weight[...])
    lay_out(proj, 2, sign(probe_gate))
    lay_out(proj, 3, sign(probe_up))
    lay_out(down, 0, down_weight[...])
    lay_out(down, 1, sign(probe_down))

    pl.semaphore_wait(barrier, len(peers))
    near = copies.slots(9)
    copies.outs(9)
    copies.send(tokens.at[other_rows], x.at[h_here, y_here, core], near, near, partner)
    copies.send(proj.at[core], proj.at[core], near + 1, near + 1, partner)
    copies.send(target.at[other_rows], tgt.at[core], near + 2, near + 2, partner)
    copies.send(down.at[core], down.at[core], near + 3, near + 3, partner)

    copies.arrived(x.at[h_here, y_here, other_core], near, partner)
    x_gather = ColGather(copies, x)
    x_gather.start()
    x_gather.spread()
    x_gather.outward()

    def token_block(ref, *place):
        return [
            ref[(*place, slice(None), half)].reshape(RING * HALF, FEATS) for half in range(2)
        ]

    row_sum = RowSum(copies, 4, part, part_landed)

    def project(index, place):
        left, right = token_block(x, place)
        both = dot_nt(proj[0, index], left) + dot_nt(proj[1, index], right)
        both = both.astype(BF16)
        part[place, 0, index] = both[:, :LANES]
        part[place, 1, index] = both[:, LANES:]

    def each(count, step):
        def body(index, carry):
            step(index)
            return carry

        lax.fori_loop(0, count, body, 0)

    def project_and_send(place):
        def one(index):
            project(index, place)
            row_sum.send_for(place, index)

        each(4, one)

    def project_first(place):
        copies.arrived(proj.at[other_core], near + 1, partner)
        project_and_send(place)

    x_gather.first(project_first)
    x_gather.middle()
    x_gather.second(project_and_send)
    x_gather.last(project_and_send)
    each(4, row_sum.forward)
    each(4, row_sum.pair)

    def strips(step):
        def body(index, carry):
            step(pl.ds(pl.multiple_of(index * STRIP, STRIP), STRIP))
            return carry

        lax.fori_loop(0, PADDED // STRIP, body, 0)

    def hide(rows):
        pre_gate, pre_up = pre[0, rows, :], pre[1, rows, :]
        act = pre_gate * jax.nn.sigmoid(pre_gate)
        hid[x_here, z_here, 0, rows, :] = (act * pre_up).astype(BF16)

    def hide_dot(rows):
        pre_gate, pre_up = pre[0, rows, :], pre[1, rows, :]
        dot_gate, dot_up = pre[2, rows, :], pre[3, rows, :]
        sig = jax.nn.sigmoid(pre_gate)
        act = pre_gate * sig
        slope = sig * (1.0 + pre_gate * (1.0 - sig))
        bend = sig * (1.0 - sig) * (2.0 + pre_gate * (1.0 - 2.0 * sig))
        hid[x_here, z_here, 1, rows, :] = (slope * dot_gate * pre_up + act * dot_up).astype(BF16)
        coef[x_here, z_here, 0, 0, rows, :] = (pre_up * slope).astype(BF16)
        coef[x_here, z_here, 0, 1, rows, :] = act.astype(BF16)
        coef[x_here, z_here, 0, 2, rows, :] = (dot_up * slope + pre_up * bend * dot_gate).astype(BF16)
        coef[x_here, z_here, 0, 3, rows, :] = (slope * dot_gate).astype(BF16)

    hid_gather = RowGather(copies, 2, hid)
    coef_gather = RowGather(copies, 1, coef)
    each(2, lambda index: row_sum.finish(pre.at[index], index))
    strips(hide)
    hid_gather.start(0)
    each(2, lambda index: row_sum.finish(pre.at[2 + index], 2 + index))
    strips(hide_dot)
    hid_gather.start(1)
    coef_gather.start_pair(0)
    layers = [(0, x_here), (1, x_minus), (2, x_plus), (3, x_opposite)]

    def out_ring(stream):
        return RingSum(
            copies,
            Y_AXIS,
            4,
            lambda place, half, layer: outs.at[stream, layer[1], place, half],
            lambda kind, layer: outs_landed.at[stream, kind, layer[0]],
            lambda kind: outs_landed.at[stream, kind],
            lambda layer: outs_landed.at[stream, pl.ds(2, 4), layer[0]],
            lambda layer: layer[0],
        )

    def layer_ring(stream):
        return RingSum(
            copies,
            H_AXIS,
            1,
            lambda place, half, index: layer_sums.at[stream, place, half],
            lambda kind, index: layer_landed.at[stream, kind],
            lambda kind: layer_landed.at[stream, kind],
            lambda index: layer_landed.at[stream, pl.ds(2, 4)],
        )

    out_sums = (out_ring(0), out_ring(1))
    layer_rings = (layer_ring(0), layer_ring(1))
    err_gathers = (ColGather(copies, err.at[0]), ColGather(copies, err.at[1]))
    back_sum = RowSum(copies, 2, back, back_landed)
    back_gather = RowGather(copies, 2, d_hid)

    def whole_units(ref, place, index):
        return jnp.concatenate([ref[place, 0, index], ref[place, 1, index]], axis=1)

    def expand(stream, layer):
        place = layer[1]
        plain = whole_units(hid, place, 0)
        for half in range(2):
            if stream == 0:
                value = dot_tn(plain, down[half, 0])
            else:
                tangent = whole_units(hid, place, 1)
                value = dot_tn(tangent, down[half, 0]) + dot_tn(plain, down[half, 1])
            value = value.astype(BF16).reshape(RING, HALF, FEATS)
            for block in range(RING):
                outs[stream, place, block, half] = value[block]
        out_sums[stream].send_opposite(layer)
        out_sums[stream].send_plus(layer)
        out_sums[stream].send_minus(layer)

    def complete(stream, layer):
        out_sum = out_sums[stream]
        out_sum.wait_terms(layer)
        for half in range(2):
            add_blocks(layer_sums.at[stream, layer[1], half], out_sum.terms(half, layer))
        layer_rings[stream].send_for(layer[1], 0)

    def settle(stream):
        ring = layer_rings[stream]
        ring.wait_terms(0)
        for half in range(2):
            add_blocks(final.at[half], ring.terms(half, 0))
            value = final[half]
            if stream == 0:
                value = value - tgt[half].astype(F32)
            err[stream, h_here, y_here, half] = value.astype(BF16)
        err_gathers[stream].start()

    def turn_back(stream):
        def one(place):
            plain = token_block(err, 0, place)
            if stream == 0:
                whole = dot_nt(down[0, 0], plain[0]) + dot_nt(down[1, 0], plain[1])
            else:
                tangent = token_block(err, 1, place)
                whole = dot_nt(down[0, 0], tangent[0]) + dot_nt(down[1, 0], tangent[1])
                whole = whole + dot_nt(down[0, 1], plain[0]) + dot_nt(down[1, 1], plain[1])
            whole = whole.astype(BF16)
            back[place, 0, stream] = whole[:, :LANES]
            back[place, 1, stream] = whole[:, LANES:]
            back_sum.send_for(place, stream)

        return one

    def slopes(place):
        for z in range(2):

            def one(rows):
                d_hidden = d_hid[place, z, 0, rows, :].astype(F32)
                for index in range(2):
                    factor = coef[place, z, 0, index, rows, :].astype(F32)
                    d_pre[place, z, index, rows, :] = (d_hidden * factor).astype(BF16)

            strips(one)

    def bends(place):
        for z in range(2):

            def one(rows):
                d_hidden = d_hid[place, z, 0, rows, :].astype(F32)
                d_hidden_dot = d_hid[place, z, 1, rows, :].astype(F32)
                for index in range(2):
                    factor = coef[place, z, 0, index, rows, :].astype(F32)
                    bent = coef[place, z, 0, 2 + index, rows, :].astype(F32)
                    value = d_hidden_dot * factor + d_hidden * bent
                    d_pre[place, z, 2 + index, rows, :] = value.astype(BF16)

            strips(one)

    hid_gather.pair(0)
    copies.arrived(down.at[other_core], near + 3, partner)
    expand(0, layers[0])
    hid_gather.forward(0)
    expand(0, layers[1])
    expand(0, layers[2])
    hid_gather.pair(1)
    expand(1, layers[0])
    out_sums[0].forward(layers[0])
    hid_gather.forward(1)
    expand(1, layers[1])
    expand(1, layers[2])
    coef_gather.start_ring(0)
    hid_gather.finish(0)
    expand(0, layers[3])
    complete(0, layers[0])
    out_sums[0].forward(layers[1])
    out_sums[0].forward(layers[2])
    out_sums[1].forward(layers[0])
    hid_gather.finish(1)
    expand(1, layers[3])
    out_sums[0].forward(layers[3])
    complete(0, layers[1])
    complete(0, layers[2])
    complete(1, layers[0])
    out_sums[1].forward(layers[1])
    out_sums[1].forward(layers[2])
    complete(0, layers[3])
    coef_gather.pair(0)
    layer_rings[0].forward(0)
    out_sums[1].forward(layers[3])
    complete(1, layers[1])
    complete(1, layers[2])
    copies.arrived(tgt.at[other_core], near + 2, partner)
    settle(0)
    complete(1, layers[3])
    layer_rings[1].forward(0)
    err_gathers[0].spread()
    err_gathers[0].outward()
    settle(1)
    coef_gather.forward(0)
    err_gathers[0].first(turn_back(0))
    err_gathers[0].middle()
    err_gathers[1].spread()
    err_gathers[1].outward()
    err_gathers[0].second(turn_back(0))
    err_gathers[1].first(turn_back(1))
    err_gathers[1].middle()
    err_gathers[0].last(turn_back(0))
    err_gathers[1].second(turn_back(1))
    back_sum.forward(0)
    err_gathers[1].last(turn_back(1))
    back_sum.pair(0)
    back_sum.forward(1)
    back_sum.finish(d_hid.at[x_here, z_here, 0], 0)
    back_gather.start(0)
    back_sum.pair(1)
    back_gather.pair(0)
    back_sum.finish(d_hid.at[x_here, z_here, 1], 1)
    back_gather.start(1)
    back_gather.forward(0)
    back_gather.pair(1)
    coef_gather.finish(0)

    def down_grads(side):
        plain_sum = jnp.zeros((PADDED, FEATS), F32)
        along_sum = jnp.zeros((PADDED, FEATS), F32)
        for place in range(RING):
            plain = whole_units(hid, place, 0)
            tangent = whole_units(hid, place, 1)
            err_block = err[0, place, :, side].reshape(RING * HALF, FEATS)
            dot_block = err[1, place, :, side].reshape(RING * HALF, FEATS)
            plain_sum = plain_sum + dot_nn(plain, err_block)
            along_sum = along_sum + dot_nn(tangent, err_block) + dot_nn(plain, dot_block)
        grads_down[side, 0] = plain_sum
        grads_down[side, 1] = along_sum

    down_grads(other_core)
    copies.send(grads_down.at[other_core], grads_down_landed, near + 4, near + 4, partner)
    down_grads(core)

    def tokens_of(place, side):
        return x[place, :, side].reshape(RING * HALF, FEATS)

    def first_grads(side, index):
        total = dot_nn(whole_units(d_pre, x_here, index), tokens_of(x_here, side))
        for place in (x_minus, x_plus):
            total = total + dot_nn(whole_units(d_pre, place, index), tokens_of(place, side))
        grads[side, index] = total

    def last_grads(side, index):
        last = dot_nn(whole_units(d_pre, x_opposite, index), tokens_of(x_opposite, side))
        grads[side, index] = grads[side, index] + last

    def last_and_send(index):
        last_grads(other_core, index)
        copies.send(grads.at[other_core, index], grads_landed.at[index], near + 5 + index, near + 5 + index, partner)
        last_grads(core, index)

    def first_both(index):
        first_grads(other_core, index)
        first_grads(core, index)

    def squares(values):
        return jnp.sum(values * values, axis=0, keepdims=True)

    outputs = (grad_gate_out, grad_up_out, grad_down_out, curv_gate_out, curv_up_out, curv_down_out)

    def to_output(index):
        return pltpu.make_async_copy(results.at[index], outputs[index], out_sems.at[index])

    def give(index, values):
        results[index] = values[:UNITS]
        to_output(index).start()

    for place in (x_here, x_minus, x_plus):
        slopes(place)
    each(2, first_both)
    back_gather.forward(1)
    back_gather.finish(0)
    slopes(x_opposite)
    each(2, last_and_send)
    for place in (x_here, x_minus, x_plus):
        bends(place)
    each(2, lambda index: first_both(2 + index))
    back_gather.finish(1)
    bends(x_opposite)
    each(2, lambda index: last_and_send(2 + index))

    copies.arrived(grads_down_landed, near + 4, partner)
    grad = grads_down[core, 0] + grads_down_landed[0]
    hess = grads_down[core, 1] + grads_down_landed[1]
    give(2, grad)
    grad_sum = squares(grad)
    curv = curvature(down[core, 1].astype(F32), hess)
    give(5, curv)
    curv_sum = squares(curv)

    for index in range(2):
        copies.arrived(grads_landed.at[index], near + 5 + index, partner)
        grad = grads[core, index] + grads_landed[index]
        give(index, grad)
        grad_sum = grad_sum + squares(grad)
    for index in range(2):
        copies.arrived(grads_landed.at[2 + index], near + 7 + index, partner)
        hess = grads[core, 2 + index] + grads_landed[2 + index]
        curv = curvature(proj[core, 2 + index].astype(F32), hess)
        give(3 + index, curv)
        curv_sum = curv_sum + squares(curv)

    lane = lax.broadcasted_iota(jnp.int32, (8, LANES), 1)
    grad_sum = jnp.sum(grad_sum, axis=1, keepdims=True)
    curv_sum = jnp.sum(curv_sum, axis=1, keepdims=True)
    tiles[0] = jnp.where(lane == 0, grad_sum, jnp.where(lane == 1, curv_sum, 0.0))

    stages = (row_peers, col_peers)
    small, small_out = copies.slots(2), copies.outs(2)
    for stage, receivers in enumerate(stages):
        for index, peer in enumerate(receivers):
            landed = tiles_landed.at[stage, index]
            copies.send(tiles.at[stage], landed, small_out + stage, small + stage, peer)
        copies.arrived(tiles_landed.at[stage], small + stage, partner)
        total = tiles[stage]
        for index in range(len(receivers)):
            total = total + tiles_landed[stage, index]
        tiles[stage + 1] = total
    sums_out[...] = tiles[len(stages)]

    assert (copies.next_out, copies.next_in) == (SENDS, ARRIVALS), (copies.next_out, copies.next_in)
    for index in range(len(outputs)):
        to_output(index).wait()
    copies.sent(x.at[0, 0, 0], near, partner)
    copies.sent(proj.at[0], near + 1, partner)
    copies.sent(tgt.at[0], near + 2, partner)
    copies.sent(down.at[0], near + 3, partner)
    copies.sent(grads_down_landed, near + 4, partner)
    each(4, lambda index: copies.sent(grads_landed.at[index], near + 5 + index, partner))
    x_gather.drain()
    err_gathers[0].drain()
    err_gathers[1].drain()
    row_sum.drain()
    back_sum.drain()
    hid_gather.drain()
    coef_gather.drain()
    back_gather.drain()
    for stream in range(2):
        out_sums[stream].drain()
        layer_rings[stream].drain()
    for stage in range(2):
        copies.sent(tiles_landed.at[stage], small_out + stage, partner)


SENDS = 94
ARRIVALS = 160


def whole_step(*operands):
    units = (PADDED, LANES)
    block = (2, HALF, FEATS)
    return pl.pallas_call(
        step_kernel,
        out_shape=(
            *[jax.ShapeDtypeStruct((UNITS, FEATS), F32)] * 6,
            jax.ShapeDtypeStruct((8, LANES), F32),
        ),
        in_specs=[pl.BlockSpec(memory_space=pltpu.VMEM)] * 8,
        out_specs=[pl.BlockSpec(memory_space=pl.ANY)] * 6 + [pl.BlockSpec(memory_space=pltpu.VMEM)],
        scratch_shapes=[
            pltpu.VMEM((2, 4, PADDED, FEATS), BF16),
            pltpu.VMEM((2, 2, PADDED, FEATS), BF16),
            pltpu.VMEM((RING, RING, *block), BF16),
            pltpu.VMEM(block, BF16),
            pltpu.VMEM((RING, 2, 4, *units), BF16),
            pltpu.VMEM((7, 4, *units), BF16),
            pltpu.VMEM((4, *units), F32),
            pltpu.VMEM((RING, 2, 2, *units), BF16),
            pltpu.VMEM((2, RING, RING, *block), BF16),
            pltpu.VMEM((2, 6, RING, HALF, FEATS), BF16),
            pltpu.VMEM((2, RING, *block), BF16),
            pltpu.VMEM((2, 6, HALF, FEATS), BF16),
            pltpu.VMEM(block, F32),
            pltpu.VMEM((2, RING, RING, *block), BF16),
            pltpu.VMEM((RING, 2, 2, *units), BF16),
            pltpu.VMEM((7, 2, *units), BF16),
            pltpu.VMEM((RING, 2, 2, *units), BF16),
            pltpu.VMEM((RING, 2, 1, 4, *units), BF16),
            pltpu.VMEM((RING, 2, 4, *units), BF16),
            pltpu.VMEM((2, 4, PADDED, FEATS), F32),
            pltpu.VMEM((4, PADDED, FEATS), F32),
            pltpu.VMEM((2, 2, PADDED, FEATS), F32),
            pltpu.VMEM((2, PADDED, FEATS), F32),
            pltpu.VMEM((3, 8, LANES), F32),
            pltpu.VMEM((2, 15, 8, LANES), F32),
            pltpu.VMEM((6, UNITS, FEATS), F32),
            pltpu.SemaphoreType.DMA((SENDS,)),
            pltpu.SemaphoreType.DMA((ARRIVALS,)),
            pltpu.SemaphoreType.DMA((6,)),
        ],
        compiler_params=pltpu.CompilerParams(
            collective_id=0, has_side_effects=True, vmem_limit_bytes=60 * 1024 * 1024
        ),
    )(*operands)


def update_kernel(sums, *refs):
    given, results = refs[:12], refs[12:21]
    loaded, computed, load_sems, store_sems = refs[21:]
    loads = [
        pltpu.make_async_copy(ref, loaded.at[index], load_sems.at[index])
        for index, ref in enumerate(given)
    ]
    stores = [
        pltpu.make_async_copy(computed.at[index], ref, store_sems.at[index])
        for index, ref in enumerate(results)
    ]
    for weight in range(3):
        for load in loads[weight::3]:
            load.start()
    count = 3.0 * D * FF
    rms_grad = jnp.sqrt(sums[0:1, 0:1] / count + 1e-06)
    rms_curv = jnp.sqrt(sums[0:1, 1:2] / count + 1e-06)
    fix_first = 1.0 - 0.9**STEP
    fix_second = 1.0 - 0.95**STEP
    for weight in range(3):
        for load in loads[weight::3]:
            load.wait()
        grad, curv, first, second = (loaded[index] for index in range(weight, 12, 3))
        new_first = 0.9 * first + 0.1 * (grad / rms_grad)
        scaled = curv / rms_curv
        new_second = 0.95 * second + 0.05 * (scaled * scaled)
        computed[weight] = new_first
        computed[3 + weight] = new_second
        computed[6 + weight] = new_first / fix_first / (jnp.sqrt(new_second / fix_second) + 1e-08)
        for store in stores[weight::3]:
            store.start()
    for store in stores:
        store.wait()


def update(sums, *arrays):
    anywhere = pl.BlockSpec(memory_space=pl.ANY)
    return pl.pallas_call(
        update_kernel,
        out_shape=[jax.ShapeDtypeStruct((UNITS, FEATS), F32)] * 9,
        in_specs=[pl.BlockSpec(memory_space=pltpu.VMEM)] + [anywhere] * 12,
        out_specs=[anywhere] * 9,
        scratch_shapes=[
            pltpu.VMEM((12, UNITS, FEATS), F32),
            pltpu.VMEM((9, UNITS, FEATS), F32),
            pltpu.SemaphoreType.DMA((12,)),
            pltpu.SemaphoreType.DMA((9,)),
        ],
        compiler_params=pltpu.CompilerParams(vmem_limit_bytes=62 * 1024 * 1024),
    )(sums, *arrays)


def body(
    tokens,
    target,
    gate_weight,
    up_weight,
    down_weight,
    probe_gate,
    probe_up,
    probe_down,
    first_gate,
    first_up,
    first_down,
    second_gate,
    second_up,
    second_down,
):
    *arrays, sums = whole_step(
        tokens, target, gate_weight.T, up_weight.T, down_weight, probe_gate.T, probe_up.T, probe_down
    )
    outs = update(
        sums, *arrays, first_gate.T, first_up.T, first_down, second_gate.T, second_up.T, second_down
    )
    return tuple(value if index % 3 == 2 else value.T for index, value in enumerate(outs))


def solution(mesh):
    torus = Mesh(mesh.devices.reshape(4, 2, 2, 4, 4), (*ROW, *COL))
    feats, units = P(ROW, COL), P(COL, ROW)
    in_specs = (units, units, feats, feats, units) + (feats, feats, units) * 3
    out_specs = (feats, feats, units) * 3
    return jax.shard_map(body, mesh=torus, in_specs=in_specs, out_specs=out_specs, check_vma=False)
```

```python
import jax
import jax.numpy as jnp
from jax import lax
from jax.experimental import pallas as pl
from jax.experimental.pallas import tpu as pltpu
from jax.sharding import Mesh
from jax.sharding import PartitionSpec as P

D = 4096
FF = 5504
STEP = 10
COL = ("col_0", "col_1")
ROW = ("row_0", "row_1", "row_2")
RING = 4
UNITS = 344
PADDED = 352
FEATS = 256
HALF = 64
LANES = 128
STRIP = 32
MESH = pl.DeviceIdType.MESH
BF16 = jnp.bfloat16
F32 = jnp.float32

X_AXIS, Z_AXIS, CORE_AXIS = ROW
H_AXIS, Y_AXIS = COL


def dot_nn(left, right):
    return jnp.dot(left, right, preferred_element_type=F32)


def dot_nt(left, right):
    return lax.dot_general(left, right, (((1,), (1,)), ((), ())), preferred_element_type=F32)


def dot_tn(left, right):
    return lax.dot_general(left, right, (((0,), (0,)), ((), ())), preferred_element_type=F32)


def block_ones(size):
    rows = lax.broadcasted_iota(jnp.int32, (size, size), 0) >> 2
    cols = lax.broadcasted_iota(jnp.int32, (size, size), 1) >> 2
    return jnp.where(rows == cols, 1.0, 0.0).astype(BF16)


def two_terms(values):
    high = values.astype(BF16)
    low = (values - high.astype(F32)).astype(BF16)
    return high, low


def curvature(sign, hess):
    high, low = two_terms(jnp.abs(sign * hess))
    ones = block_ones(hess.shape[0])
    down = dot_nn(ones, high) + dot_nn(ones, low)
    high, low = two_terms(down)
    ones = block_ones(hess.shape[1])
    return (dot_nn(high, ones) + dot_nn(low, ones)) * 0.0625


class Copies:
    def __init__(self, send_sems, recv_sems):
        self.send_sems = send_sems
        self.recv_sems = recv_sems
        self.next_in = 0
        self.next_out = 0

    def slots(self, count):
        self.next_in += count
        return self.next_in - count

    def outs(self, count):
        self.next_out += count
        return self.next_out - count

    def copy(self, src, dst, out, slot, peer):
        return pltpu.make_async_remote_copy(
            src_ref=src,
            dst_ref=dst,
            send_sem=self.send_sems.at[out],
            recv_sem=self.recv_sems.at[slot],
            device_id=peer,
            device_id_type=MESH,
        )

    def send(self, src, dst, out, slot, peer):
        self.copy(src, dst, out, slot, peer).start()

    def arrived(self, dst, slot, peer):
        self.copy(dst, dst, 0, slot, peer).wait_recv()

    def sent(self, src, out, peer):
        self.copy(src, src, out, 0, peer).wait_send()


def around(axis):
    here = lax.axis_index(axis)
    return here, lax.rem(here + 1, RING), lax.rem(here + 3, RING), lax.rem(here + 2, RING)


def add_strips(dst, terms):
    def strip(index, carry):
        rows = pl.ds(pl.multiple_of(index * STRIP, STRIP), STRIP)
        total = terms[0][rows, :].astype(F32)
        for term in terms[1:]:
            total = total + term[rows, :].astype(F32)
        dst[rows, :] = total.astype(dst.dtype)
        return carry

    lax.fori_loop(0, PADDED // STRIP, strip, 0)


def add_blocks(dst, terms):
    total = terms[0][...].astype(F32)
    for term in terms[1:]:
        total = total + term[...].astype(F32)
    dst[...] = total.astype(dst.dtype)


class RingSum:
    def __init__(self, copies, axis, count, block, landed, all_landed, last, number=lambda index: index):
        self.last = last
        self.number, self.all_landed = number, all_landed
        self.out = copies.outs(6)
        self.copies, self.axis, self.block, self.landed = copies, axis, block, landed
        self.base = copies.slots(3 * count)
        self.count = count
        self.here, self.plus, self.minus, self.opposite = around(axis)

    def slot(self, kind, index):
        return self.base + min(kind, 2) * self.count + self.number(index)

    def send(self, src, kind, index, peer):
        slot = self.slot(kind, index)
        self.copies.send(src, self.landed(kind, index), self.out + kind, slot, {self.axis: peer})

    def wait(self, kind, index):
        ref = self.landed(kind, index)
        self.copies.arrived(ref, self.slot(kind, index), {self.axis: self.plus})

    def send_for(self, place, index):
        role = lax.rem(place - self.here + RING, RING)

        @pl.when(role == 1)
        def _():
            self.send(self.block(place, 1, index), 3, index, self.plus)

        @pl.when(role == 2)
        def _():
            self.send(self.block(place, 0, index), 0, index, self.plus)
            self.send(self.block(place, 1, index), 1, index, self.minus)

        @pl.when(role == 3)
        def _():
            self.send(self.block(place, 0, index), 4, index, self.minus)

    def send_opposite(self, index):
        self.send(self.block(self.opposite, 0, index), 0, index, self.plus)
        self.send(self.block(self.opposite, 1, index), 1, index, self.minus)

    def send_plus(self, index):
        self.send(self.block(self.plus, 1, index), 3, index, self.plus)

    def send_minus(self, index):
        self.send(self.block(self.minus, 0, index), 4, index, self.minus)

    def forward(self, index):
        self.wait(0, index)
        ref = self.block(self.plus, 0, index)
        add_blocks(ref, (ref, self.landed(0, index)))
        self.send(ref, 2, index, self.plus)
        self.wait(1, index)
        ref = self.block(self.minus, 1, index)
        add_blocks(ref, (ref, self.landed(1, index)))
        self.send(ref, 5, index, self.minus)

    def wait_terms(self, index):
        self.copies.arrived(self.last(index), self.slot(2, index), {self.axis: self.plus})

    def terms(self, half, index):
        return (
            self.block(self.here, half, index),
            self.landed(2 + half, index),
            self.landed(4 + half, index),
        )

    def drain(self):
        for kind in range(6):
            self.copies.sent(self.all_landed(kind), self.out + kind, {self.axis: self.plus})


class RowSum:
    def __init__(self, copies, count, blocks, landed):
        self.copies, self.count, self.blocks, self.landed = copies, count, blocks, landed
        self.base, self.out = copies.slots(4 * count), copies.outs(7)
        self.here, self.plus, self.minus, self.opposite = around(X_AXIS)
        self.z = lax.axis_index(Z_AXIS)
        self.other = 1 - self.z

    def slot(self, kind, index):
        return self.base + (0, 1, 2, 2, 2, 2, 3)[kind] * self.count + index

    def send(self, place, half, kind, index, peer):
        src = self.blocks.at[place, half, index]
        slot = self.slot(kind, index)
        self.copies.send(src, self.landed.at[kind, index], self.out + kind, slot, peer)

    def wait(self, kind, index):
        ref = self.landed.at[pl.ds(2, 4) if kind == 2 else kind, index]
        self.copies.arrived(ref, self.slot(kind, index), {Z_AXIS: self.other})

    def send_for(self, place, index):
        role = lax.rem(place - self.here + RING, RING)

        @pl.when(role == 1)
        def _():
            self.send(place, 1, 3, index, {X_AXIS: self.plus})

        @pl.when(role == 2)
        def _():
            self.send(place, 0, 0, index, {X_AXIS: self.plus})
            self.send(place, 1, 1, index, {X_AXIS: self.minus})

        @pl.when(role == 3)
        def _():
            self.send(place, 0, 4, index, {X_AXIS: self.minus})

    def forward(self, index):
        self.wait(0, index)
        ref = self.blocks.at[self.plus, 0, index]
        add_strips(ref, (ref, self.landed.at[0, index]))
        self.send(self.plus, 0, 2, index, {X_AXIS: self.plus})
        self.wait(1, index)
        ref = self.blocks.at[self.minus, 1, index]
        add_strips(ref, (ref, self.landed.at[1, index]))
        self.send(self.minus, 1, 5, index, {X_AXIS: self.minus})

    def terms(self, half, index):
        return (
            self.blocks.at[self.here, half, index],
            self.landed.at[2 + half, index],
            self.landed.at[4 + half, index],
        )

    def pair(self, index):
        self.wait(2, index)
        add_strips(self.blocks.at[self.here, self.other, index], self.terms(self.other, index))
        self.send(self.here, self.other, 6, index, {Z_AXIS: self.other})

    def finish(self, dst, index):
        self.wait(6, index)
        add_strips(dst, (*self.terms(self.z, index), self.landed.at[6, index]))

    def drain(self):
        for kind in range(7):
            self.copies.sent(self.landed.at[kind], self.out + kind, {Z_AXIS: self.other})


class RowGather:
    def __init__(self, copies, count, buffer):
        self.copies, self.count, self.buffer = copies, count, buffer
        self.base, self.out = copies.slots(7 * count), copies.outs(7)
        self.here, self.plus, self.minus, self.opposite = around(X_AXIS)
        self.z = lax.axis_index(Z_AXIS)
        self.other = 1 - self.z

    def send(self, place, z, kind, index, peer):
        ref = self.buffer.at[place, z, index]
        slot = self.base + kind * self.count + index
        self.copies.send(ref, ref, self.out + kind, slot, peer)

    def wait(self, place, z, kind, index):
        ref = self.buffer.at[place, z, index]
        slot = self.base + kind * self.count + index
        self.copies.arrived(ref, slot, {Z_AXIS: self.other})

    def start(self, index):
        self.start_pair(index)
        self.start_ring(index)

    def start_pair(self, index):
        self.send(self.here, self.z, 0, index, {Z_AXIS: self.other})

    def start_ring(self, index):
        self.send(self.here, self.z, 1, index, {X_AXIS: self.plus})
        self.send(self.here, self.z, 2, index, {X_AXIS: self.minus})

    def pair(self, index):
        self.wait(self.here, self.other, 0, index)
        self.send(self.here, self.other, 3, index, {X_AXIS: self.plus})
        self.send(self.here, self.other, 4, index, {X_AXIS: self.minus})

    def forward(self, index):
        self.wait(self.minus, self.z, 1, index)
        self.wait(self.minus, self.other, 3, index)
        self.send(self.minus, 0, 5, index, {X_AXIS: self.plus})
        self.wait(self.plus, self.z, 2, index)
        self.wait(self.plus, self.other, 4, index)
        self.send(self.plus, 1, 6, index, {X_AXIS: self.minus})

    def finish(self, index):
        self.wait(self.opposite, 0, 5, index)
        self.wait(self.opposite, 1, 6, index)

    def drain(self):
        for kind in range(7):
            self.copies.sent(self.buffer.at[0, 0], self.out + kind, {Z_AXIS: self.other})


class RingGather:
    def __init__(self, copies, axis, whole, half, out):
        self.copies, self.axis, self.whole, self.half = copies, axis, whole, half
        self.base, self.out = copies.slots(4), out
        self.here, self.plus, self.minus, self.opposite = around(axis)

    def send(self, ref, kind, peer):
        self.copies.send(ref, ref, self.out + kind, self.base + kind, {self.axis: peer})

    def wait(self, ref, kind):
        self.copies.arrived(ref, self.base + kind, {self.axis: self.plus})

    def start(self):
        self.send(self.whole(self.here), 0, self.plus)
        self.send(self.whole(self.here), 1, self.minus)

    def from_minus(self):
        self.wait(self.whole(self.minus), 0)
        self.send(self.half(self.minus, 0), 2, self.plus)

    def from_plus(self):
        self.wait(self.whole(self.plus), 1)
        self.send(self.half(self.plus, 1), 3, self.minus)

    def forward(self):
        self.from_minus()
        self.from_plus()

    def finish(self):
        self.wait(self.half(self.opposite, 0), 2)
        self.wait(self.half(self.opposite, 1), 3)


class ColGather:
    def __init__(self, copies, buffer):
        here, plus, minus, opposite = around(H_AXIS)
        y = lax.axis_index(Y_AXIS)
        self.copies, self.buffer = copies, buffer
        self.out = copies.outs(8)
        self.outer = RingGather(
            copies,
            H_AXIS,
            lambda place: buffer.at[place, y],
            lambda place, half: buffer.at[place, y, half],
            self.out,
        )
        self.inner = [
            RingGather(
                copies,
                Y_AXIS,
                lambda place, layer=layer: buffer.at[layer, place],
                lambda place, half, layer=layer: buffer.at[layer, place, half],
                self.out + 4,
            )
            for layer in (here, minus, plus, opposite)
        ]
        self.places = (here, minus, plus, opposite)

    def start(self):
        self.outer.start()
        self.inner[0].start()

    def spread(self):
        self.inner[0].forward()

    def outward(self):
        self.outer.from_minus()
        self.inner[1].start()
        self.outer.from_plus()
        self.inner[2].start()

    def first(self, use):
        self.inner[0].finish()
        use(self.places[0])

    def middle(self):
        self.inner[1].forward()
        self.inner[2].forward()
        self.outer.finish()
        self.inner[3].start()

    def second(self, use, early):
        self.inner[1].finish()
        use(self.places[1])
        if early:
            self.inner[3].forward()
        self.inner[2].finish()
        use(self.places[2])
        if not early:
            self.inner[3].forward()

    def last(self, use):
        self.inner[3].finish()
        use(self.places[3])

    def drain(self):
        for kind in range(4):
            one = self.buffer.at[0, 0] if kind < 2 else self.buffer.at[0, 0, 0]
            all_layers = self.buffer.at[0] if kind < 2 else self.buffer.at[0, pl.ds(0, 2)]
            self.copies.sent(one, self.out + kind, {H_AXIS: self.outer.plus})
            self.copies.sent(all_layers, self.out + 4 + kind, {H_AXIS: self.outer.plus})


def step_kernel(
    tokens_in,
    target_in,
    gate_weight_in,
    up_weight_in,
    down_weight_in,
    probe_gate_in,
    probe_up_in,
    probe_down_in,
    grad_gate_out,
    grad_up_out,
    grad_down_out,
    curv_gate_out,
    curv_up_out,
    curv_down_out,
    sums_out,
    proj,
    down,
    x,
    tgt,
    part,
    part_landed,
    pre,
    hid,
    outs,
    outs_landed,
    layer_sums,
    layer_landed,
    final,
    err,
    back,
    back_landed,
    d_hid,
    coef,
    d_pre,
    grads,
    grads_landed,
    grads_down,
    grads_down_landed,
    tiles,
    tiles_landed,
    results,
    send_sems,
    recv_sems,
    out_sems,
    tokens,
    target,
    gate_weight,
    up_weight,
    down_weight,
    probe_gate,
    probe_up,
    probe_down,
    in_sems,
):
    loads = [
        pltpu.make_async_copy(src, dst, in_sems.at[index])
        for index, (src, dst) in enumerate(
            (
                (tokens_in, tokens),
                (target_in, target),
                (gate_weight_in, gate_weight),
                (up_weight_in, up_weight),
                (probe_gate_in, probe_gate),
                (probe_up_in, probe_up),
                (down_weight_in, down_weight),
                (probe_down_in, probe_down),
            )
        )
    ]
    for load in loads:
        load.start()
    copies = Copies(send_sems, recv_sems)
    core = lax.axis_index(CORE_AXIS)
    other_core = 1 - core
    x_here, x_plus, x_minus, x_opposite = around(X_AXIS)
    y_here, y_plus, y_minus, y_opposite = around(Y_AXIS)
    h_here, h_plus, h_minus, h_opposite = around(H_AXIS)
    z_here = lax.axis_index(Z_AXIS)
    partner = {CORE_AXIS: other_core}

    barrier = pltpu.get_barrier_semaphore()
    def displaced(axes, sizes):
        steps = [()]
        for size in sizes:
            steps = [(*step, more) for step in steps for more in range(size)]
        return [
            {
                axis: lax.rem(lax.axis_index(axis) + more, size)
                for axis, size, more in zip(axes, sizes, step)
            }
            for step in steps[1:]
        ]

    row_peers = displaced(ROW, (RING, 2, 2))
    col_peers = displaced(COL, (RING, RING))
    peers = row_peers + col_peers
    for peer in peers:
        pl.semaphore_signal(barrier, inc=1, device_id=peer, device_id_type=MESH)

    own_rows = pl.ds(pl.multiple_of(core * HALF, HALF), HALF)
    other_rows = pl.ds(pl.multiple_of(other_core * HALF, HALF), HALF)
    loads[0].wait()
    loads[1].wait()
    x[h_here, y_here, core] = tokens[own_rows, :]
    tgt[core] = target[own_rows, :]

    def sign(ref):
        return (2 * ref[...] - 1).astype(F32).astype(BF16)

    def lay_out(dst, index, values):
        dst[core, index, PADDED - 32 :] = jnp.zeros((32, FEATS), BF16)
        dst[core, index, :UNITS] = values

    for load in loads[2:]:
        load.wait()
    lay_out(proj, 0, gate_weight[...])
    lay_out(proj, 1, up_weight[...])
    lay_out(proj, 2, sign(probe_gate))
    lay_out(proj, 3, sign(probe_up))
    lay_out(down, 0, down_weight[...])
    lay_out(down, 1, sign(probe_down))

    pl.semaphore_wait(barrier, len(peers))
    near = copies.slots(9)
    copies.outs(9)
    copies.send(tokens.at[other_rows], x.at[h_here, y_here, core], near, near, partner)
    copies.send(proj.at[core], proj.at[core], near + 1, near + 1, partner)
    copies.send(target.at[other_rows], tgt.at[core], near + 2, near + 2, partner)
    copies.send(down.at[core], down.at[core], near + 3, near + 3, partner)

    copies.arrived(x.at[h_here, y_here, other_core], near, partner)
    x_gather = ColGather(copies, x)
    x_gather.start()
    x_gather.spread()
    x_gather.outward()

    def token_block(ref, *place):
        return [
            ref[(*place, slice(None), half)].reshape(RING * HALF, FEATS) for half in range(2)
        ]

    row_sum = RowSum(copies, 4, part, part_landed)

    def project(index, place):
        left, right = token_block(x, place)
        both = dot_nt(proj[0, index], left) + dot_nt(proj[1, index], right)
        both = both.astype(BF16)
        part[place, 0, index] = both[:, :LANES]
        part[place, 1, index] = both[:, LANES:]

    def each(count, step):
        def body(index, carry):
            step(index)
            return carry

        lax.fori_loop(0, count, body, 0)

    def project_and_send(place):
        def one(index):
            project(index, place)
            row_sum.send_for(place, index)

        each(4, one)

    def project_first(place):
        copies.arrived(proj.at[other_core], near + 1, partner)
        project_and_send(place)

    x_gather.first(project_first)
    x_gather.middle()
    x_gather.second(project_and_send, True)
    x_gather.last(project_and_send)
    each(4, row_sum.forward)
    each(4, row_sum.pair)

    def strips(step):
        def body(index, carry):
            step(pl.ds(pl.multiple_of(index * STRIP, STRIP), STRIP))
            return carry

        lax.fori_loop(0, PADDED // STRIP, body, 0)

    def hide(rows):
        pre_gate, pre_up = pre[0, rows, :], pre[1, rows, :]
        act = pre_gate * jax.nn.sigmoid(pre_gate)
        hid[x_here, z_here, 0, rows, :] = (act * pre_up).astype(BF16)

    def hide_dot(rows):
        pre_gate, pre_up = pre[0, rows, :], pre[1, rows, :]
        dot_gate, dot_up = pre[2, rows, :], pre[3, rows, :]
        sig = jax.nn.sigmoid(pre_gate)
        act = pre_gate * sig
        slope = sig * (1.0 + pre_gate * (1.0 - sig))
        bend = sig * (1.0 - sig) * (2.0 + pre_gate * (1.0 - 2.0 * sig))
        hid[x_here, z_here, 1, rows, :] = (slope * dot_gate * pre_up + act * dot_up).astype(BF16)
        coef[x_here, z_here, 0, 0, rows, :] = (pre_up * slope).astype(BF16)
        coef[x_here, z_here, 0, 1, rows, :] = act.astype(BF16)
        coef[x_here, z_here, 0, 2, rows, :] = (dot_up * slope + pre_up * bend * dot_gate).astype(BF16)
        coef[x_here, z_here, 0, 3, rows, :] = (slope * dot_gate).astype(BF16)

    hid_gather = RowGather(copies, 2, hid)
    coef_gather = RowGather(copies, 1, coef)
    each(2, lambda index: row_sum.finish(pre.at[index], index))
    strips(hide)
    hid_gather.start(0)
    each(2, lambda index: row_sum.finish(pre.at[2 + index], 2 + index))
    strips(hide_dot)
    hid_gather.start(1)
    coef_gather.start_pair(0)
    layers = [(0, x_here), (1, x_minus), (2, x_plus), (3, x_opposite)]

    def out_ring(stream):
        return RingSum(
            copies,
            Y_AXIS,
            4,
            lambda place, half, layer: outs.at[stream, layer[1], place, half],
            lambda kind, layer: outs_landed.at[stream, kind, layer[0]],
            lambda kind: outs_landed.at[stream, kind],
            lambda layer: outs_landed.at[stream, pl.ds(2, 4), layer[0]],
            lambda layer: layer[0],
        )

    def layer_ring(stream):
        return RingSum(
            copies,
            H_AXIS,
            1,
            lambda place, half, index: layer_sums.at[stream, place, half],
            lambda kind, index: layer_landed.at[stream, kind],
            lambda kind: layer_landed.at[stream, kind],
            lambda index: layer_landed.at[stream, pl.ds(2, 4)],
        )

    out_sums = (out_ring(0), out_ring(1))
    layer_rings = (layer_ring(0), layer_ring(1))
    err_gathers = (ColGather(copies, err.at[0]), ColGather(copies, err.at[1]))
    back_sum = RowSum(copies, 2, back, back_landed)
    back_gather = RowGather(copies, 2, d_hid)

    def whole_units(ref, place, index):
        return jnp.concatenate([ref[place, 0, index], ref[place, 1, index]], axis=1)

    def expand(stream, layer):
        place = layer[1]
        plain = whole_units(hid, place, 0)
        for half in range(2):
            if stream == 0:
                value = dot_tn(plain, down[half, 0])
            else:
                tangent = whole_units(hid, place, 1)
                value = dot_tn(tangent, down[half, 0]) + dot_tn(plain, down[half, 1])
            value = value.astype(BF16).reshape(RING, HALF, FEATS)
            for block in range(RING):
                outs[stream, place, block, half] = value[block]
        out_sums[stream].send_opposite(layer)
        out_sums[stream].send_plus(layer)
        out_sums[stream].send_minus(layer)

    def complete(stream, layer):
        out_sum = out_sums[stream]
        out_sum.wait_terms(layer)
        for half in range(2):
            add_blocks(layer_sums.at[stream, layer[1], half], out_sum.terms(half, layer))
        layer_rings[stream].send_for(layer[1], 0)

    def settle(stream):
        ring = layer_rings[stream]
        ring.wait_terms(0)
        for half in range(2):
            add_blocks(final.at[half], ring.terms(half, 0))
            value = final[half]
            if stream == 0:
                value = value - tgt[half].astype(F32)
            err[stream, h_here, y_here, half] = value.astype(BF16)
        err_gathers[stream].start()

    def turn_back(stream):
        def one(place):
            plain = token_block(err, 0, place)
            if stream == 0:
                whole = dot_nt(down[0, 0], plain[0]) + dot_nt(down[1, 0], plain[1])
            else:
                tangent = token_block(err, 1, place)
                whole = dot_nt(down[0, 0], tangent[0]) + dot_nt(down[1, 0], tangent[1])
                whole = whole + dot_nt(down[0, 1], plain[0]) + dot_nt(down[1, 1], plain[1])
            whole = whole.astype(BF16)
            back[place, 0, stream] = whole[:, :LANES]
            back[place, 1, stream] = whole[:, LANES:]
            back_sum.send_for(place, stream)

        return one

    def slopes(place):
        for z in range(2):

            def one(rows):
                d_hidden = d_hid[place, z, 0, rows, :].astype(F32)
                for index in range(2):
                    factor = coef[place, z, 0, index, rows, :].astype(F32)
                    d_pre[place, z, index, rows, :] = (d_hidden * factor).astype(BF16)

            strips(one)

    def bends(place):
        for z in range(2):

            def one(rows):
                d_hidden = d_hid[place, z, 0, rows, :].astype(F32)
                d_hidden_dot = d_hid[place, z, 1, rows, :].astype(F32)
                for index in range(2):
                    factor = coef[place, z, 0, index, rows, :].astype(F32)
                    bent = coef[place, z, 0, 2 + index, rows, :].astype(F32)
                    value = d_hidden_dot * factor + d_hidden * bent
                    d_pre[place, z, 2 + index, rows, :] = value.astype(BF16)

            strips(one)

    def down_grads(side):
        plain_sum = jnp.zeros((PADDED, FEATS), F32)
        along_sum = jnp.zeros((PADDED, FEATS), F32)
        for place in range(RING):
            plain = whole_units(hid, place, 0)
            tangent = whole_units(hid, place, 1)
            err_block = err[0, place, :, side].reshape(RING * HALF, FEATS)
            dot_block = err[1, place, :, side].reshape(RING * HALF, FEATS)
            plain_sum = plain_sum + dot_nn(plain, err_block)
            along_sum = along_sum + dot_nn(tangent, err_block) + dot_nn(plain, dot_block)
        grads_down[side, 0] = plain_sum
        grads_down[side, 1] = along_sum

    hid_gather.pair(0)
    copies.arrived(down.at[other_core], near + 3, partner)
    expand(0, layers[0])
    hid_gather.forward(0)
    expand(0, layers[1])
    expand(0, layers[2])
    hid_gather.pair(1)
    expand(1, layers[0])
    out_sums[0].forward(layers[0])
    hid_gather.forward(1)
    expand(1, layers[1])
    expand(1, layers[2])
    coef_gather.start_ring(0)
    hid_gather.finish(0)
    expand(0, layers[3])
    complete(0, layers[0])
    out_sums[0].forward(layers[1])
    out_sums[0].forward(layers[2])
    out_sums[1].forward(layers[0])
    hid_gather.finish(1)
    expand(1, layers[3])
    out_sums[0].forward(layers[3])
    complete(0, layers[1])
    complete(0, layers[2])
    complete(1, layers[0])
    out_sums[1].forward(layers[1])
    out_sums[1].forward(layers[2])
    complete(0, layers[3])
    coef_gather.pair(0)
    layer_rings[0].forward(0)
    out_sums[1].forward(layers[3])
    complete(1, layers[1])
    complete(1, layers[2])
    copies.arrived(tgt.at[other_core], near + 2, partner)
    settle(0)
    complete(1, layers[3])
    layer_rings[1].forward(0)
    err_gathers[0].spread()
    err_gathers[0].outward()
    settle(1)
    coef_gather.forward(0)
    err_gathers[0].first(turn_back(0))
    err_gathers[0].middle()
    err_gathers[1].spread()
    err_gathers[1].outward()
    err_gathers[0].second(turn_back(0), False)
    err_gathers[1].first(turn_back(1))
    err_gathers[1].middle()
    err_gathers[0].last(turn_back(0))
    err_gathers[1].second(turn_back(1), False)
    back_sum.forward(0)
    err_gathers[1].last(turn_back(1))
    back_sum.pair(0)
    back_sum.forward(1)
    down_grads(other_core)
    copies.send(grads_down.at[other_core], grads_down_landed, near + 4, near + 4, partner)
    back_sum.finish(d_hid.at[x_here, z_here, 0], 0)
    back_gather.start(0)
    down_grads(core)
    back_sum.pair(1)
    back_gather.pair(0)
    back_sum.finish(d_hid.at[x_here, z_here, 1], 1)
    back_gather.start(1)
    back_gather.forward(0)
    back_gather.pair(1)
    coef_gather.finish(0)


    def tokens_of(place, side):
        return x[place, :, side].reshape(RING * HALF, FEATS)

    def first_grads(side, index):
        total = dot_nn(whole_units(d_pre, x_here, index), tokens_of(x_here, side))
        for place in (x_minus, x_plus):
            total = total + dot_nn(whole_units(d_pre, place, index), tokens_of(place, side))
        grads[side, index] = total

    def last_grads(side, index):
        last = dot_nn(whole_units(d_pre, x_opposite, index), tokens_of(x_opposite, side))
        grads[side, index] = grads[side, index] + last

    def last_and_send(index):
        last_grads(other_core, index)
        copies.send(grads.at[other_core, index], grads_landed.at[index], near + 5 + index, near + 5 + index, partner)
        last_grads(core, index)

    def first_both(index):
        first_grads(other_core, index)
        first_grads(core, index)

    def squares(values):
        return jnp.sum(values * values, axis=0, keepdims=True)

    outputs = (grad_gate_out, grad_up_out, grad_down_out, curv_gate_out, curv_up_out, curv_down_out)

    def to_output(index):
        return pltpu.make_async_copy(results.at[index], outputs[index], out_sems.at[index])

    def give(index, values):
        results[index] = values[:UNITS]
        to_output(index).start()

    for place in (x_here, x_minus, x_plus):
        slopes(place)
    each(2, first_both)
    back_gather.forward(1)
    back_gather.finish(0)
    slopes(x_opposite)
    each(2, last_and_send)
    for place in (x_here, x_minus, x_plus):
        bends(place)
    each(2, lambda index: first_both(2 + index))
    back_gather.finish(1)
    bends(x_opposite)
    each(2, lambda index: last_and_send(2 + index))

    copies.arrived(grads_down_landed, near + 4, partner)
    grad = grads_down[core, 0] + grads_down_landed[0]
    hess = grads_down[core, 1] + grads_down_landed[1]
    give(2, grad)
    grad_sum = squares(grad)
    curv = curvature(down[core, 1].astype(F32), hess)
    give(5, curv)
    curv_sum = squares(curv)

    for index in range(2):
        copies.arrived(grads_landed.at[index], near + 5 + index, partner)
        grad = grads[core, index] + grads_landed[index]
        give(index, grad)
        grad_sum = grad_sum + squares(grad)
    for index in range(2):
        copies.arrived(grads_landed.at[2 + index], near + 7 + index, partner)
        hess = grads[core, 2 + index] + grads_landed[2 + index]
        curv = curvature(proj[core, 2 + index].astype(F32), hess)
        give(3 + index, curv)
        curv_sum = curv_sum + squares(curv)

    lane = lax.broadcasted_iota(jnp.int32, (8, LANES), 1)
    grad_sum = jnp.sum(grad_sum, axis=1, keepdims=True)
    curv_sum = jnp.sum(curv_sum, axis=1, keepdims=True)
    tiles[0] = jnp.where(lane == 0, grad_sum, jnp.where(lane == 1, curv_sum, 0.0))

    stages = (row_peers, col_peers)
    small, small_out = copies.slots(2), copies.outs(2)
    for stage, receivers in enumerate(stages):
        for index, peer in enumerate(receivers):
            landed = tiles_landed.at[stage, index]
            copies.send(tiles.at[stage], landed, small_out + stage, small + stage, peer)
        copies.arrived(tiles_landed.at[stage], small + stage, partner)
        total = tiles[stage]
        for index in range(len(receivers)):
            total = total + tiles_landed[stage, index]
        tiles[stage + 1] = total
    sums_out[...] = tiles[len(stages)]

    assert (copies.next_out, copies.next_in) == (SENDS, ARRIVALS), (copies.next_out, copies.next_in)
    for index in range(len(outputs)):
        to_output(index).wait()
    copies.sent(x.at[0, 0, 0], near, partner)
    copies.sent(proj.at[0], near + 1, partner)
    copies.sent(tgt.at[0], near + 2, partner)
    copies.sent(down.at[0], near + 3, partner)
    copies.sent(grads_down_landed, near + 4, partner)
    each(4, lambda index: copies.sent(grads_landed.at[index], near + 5 + index, partner))
    x_gather.drain()
    err_gathers[0].drain()
    err_gathers[1].drain()
    row_sum.drain()
    back_sum.drain()
    hid_gather.drain()
    coef_gather.drain()
    back_gather.drain()
    for stream in range(2):
        out_sums[stream].drain()
        layer_rings[stream].drain()
    for stage in range(2):
        copies.sent(tiles_landed.at[stage], small_out + stage, partner)


SENDS = 94
ARRIVALS = 160


def whole_step(*operands):
    units = (PADDED, LANES)
    block = (2, HALF, FEATS)
    return pl.pallas_call(
        step_kernel,
        out_shape=(
            *[jax.ShapeDtypeStruct((UNITS, FEATS), F32)] * 6,
            jax.ShapeDtypeStruct((8, LANES), F32),
        ),
        in_specs=[pl.BlockSpec(memory_space=pl.ANY)] * 8,
        out_specs=[pl.BlockSpec(memory_space=pl.ANY)] * 6 + [pl.BlockSpec(memory_space=pltpu.VMEM)],
        scratch_shapes=[
            pltpu.VMEM((2, 4, PADDED, FEATS), BF16),
            pltpu.VMEM((2, 2, PADDED, FEATS), BF16),
            pltpu.VMEM((RING, RING, *block), BF16),
            pltpu.VMEM(block, BF16),
            pltpu.VMEM((RING, 2, 4, *units), BF16),
            pltpu.VMEM((7, 4, *units), BF16),
            pltpu.VMEM((4, *units), F32),
            pltpu.VMEM((RING, 2, 2, *units), BF16),
            pltpu.VMEM((2, RING, RING, *block), BF16),
            pltpu.VMEM((2, 6, RING, HALF, FEATS), BF16),
            pltpu.VMEM((2, RING, *block), BF16),
            pltpu.VMEM((2, 6, HALF, FEATS), BF16),
            pltpu.VMEM(block, F32),
            pltpu.VMEM((2, RING, RING, *block), BF16),
            pltpu.VMEM((RING, 2, 2, *units), BF16),
            pltpu.VMEM((7, 2, *units), BF16),
            pltpu.VMEM((RING, 2, 2, *units), BF16),
            pltpu.VMEM((RING, 2, 1, 4, *units), BF16),
            pltpu.VMEM((RING, 2, 4, *units), BF16),
            pltpu.VMEM((2, 4, PADDED, FEATS), F32),
            pltpu.VMEM((4, PADDED, FEATS), F32),
            pltpu.VMEM((2, 2, PADDED, FEATS), F32),
            pltpu.VMEM((2, PADDED, FEATS), F32),
            pltpu.VMEM((3, 8, LANES), F32),
            pltpu.VMEM((2, 15, 8, LANES), F32),
            pltpu.VMEM((6, UNITS, FEATS), F32),
            pltpu.SemaphoreType.DMA((SENDS,)),
            pltpu.SemaphoreType.DMA((ARRIVALS,)),
            pltpu.SemaphoreType.DMA((6,)),
            *[pltpu.VMEM(operand.shape, operand.dtype) for operand in operands],
            pltpu.SemaphoreType.DMA((8,)),
        ],
        compiler_params=pltpu.CompilerParams(
            collective_id=0, has_side_effects=True, vmem_limit_bytes=60 * 1024 * 1024
        ),
    )(*operands)


def update_kernel(sums, *refs):
    given, results = refs[:12], refs[12:21]
    loaded, computed, load_sems, store_sems = refs[21:]
    loads = [
        pltpu.make_async_copy(ref, loaded.at[index], load_sems.at[index])
        for index, ref in enumerate(given)
    ]
    stores = [
        pltpu.make_async_copy(computed.at[index], ref, store_sems.at[index])
        for index, ref in enumerate(results)
    ]
    for weight in range(3):
        for load in loads[weight::3]:
            load.start()
    count = 3.0 * D * FF
    rms_grad = jnp.sqrt(sums[0:1, 0:1] / count + 1e-06)
    rms_curv = jnp.sqrt(sums[0:1, 1:2] / count + 1e-06)
    fix_first = 1.0 - 0.9**STEP
    fix_second = 1.0 - 0.95**STEP
    for weight in range(3):
        for load in loads[weight::3]:
            load.wait()
        grad, curv, first, second = (loaded[index] for index in range(weight, 12, 3))
        new_first = 0.9 * first + 0.1 * (grad / rms_grad)
        scaled = curv / rms_curv
        new_second = 0.95 * second + 0.05 * (scaled * scaled)
        computed[weight] = new_first
        computed[3 + weight] = new_second
        computed[6 + weight] = new_first / fix_first / (jnp.sqrt(new_second / fix_second) + 1e-08)
        for store in stores[weight::3]:
            store.start()
    for store in stores:
        store.wait()


def update(sums, *arrays):
    anywhere = pl.BlockSpec(memory_space=pl.ANY)
    return pl.pallas_call(
        update_kernel,
        out_shape=[jax.ShapeDtypeStruct((UNITS, FEATS), F32)] * 9,
        in_specs=[pl.BlockSpec(memory_space=pltpu.VMEM)] + [anywhere] * 12,
        out_specs=[anywhere] * 9,
        scratch_shapes=[
            pltpu.VMEM((12, UNITS, FEATS), F32),
            pltpu.VMEM((9, UNITS, FEATS), F32),
            pltpu.SemaphoreType.DMA((12,)),
            pltpu.SemaphoreType.DMA((9,)),
        ],
        compiler_params=pltpu.CompilerParams(vmem_limit_bytes=62 * 1024 * 1024),
    )(sums, *arrays)


def body(
    tokens,
    target,
    gate_weight,
    up_weight,
    down_weight,
    probe_gate,
    probe_up,
    probe_down,
    first_gate,
    first_up,
    first_down,
    second_gate,
    second_up,
    second_down,
):
    *arrays, sums = whole_step(
        tokens, target, gate_weight.T, up_weight.T, down_weight, probe_gate.T, probe_up.T, probe_down
    )
    outs = update(
        sums, *arrays, first_gate.T, first_up.T, first_down, second_gate.T, second_up.T, second_down
    )
    return tuple(value if index % 3 == 2 else value.T for index, value in enumerate(outs))


def solution(mesh):
    torus = Mesh(mesh.devices.reshape(4, 2, 2, 4, 4), (*ROW, *COL))
    feats, units = P(ROW, COL), P(COL, ROW)
    in_specs = (units, units, feats, feats, units) + (feats, feats, units) * 3
    out_specs = (feats, feats, units) * 3
    return jax.shard_map(body, mesh=torus, in_specs=in_specs, out_specs=out_specs, check_vma=False)
```
